128 devices in a mesh: gx: 16 (over z, y_lo, core), gy: 8 (over y_hi, x).
Axes of the slice: x: 4, y: 4 (y_hi: 2, y_lo: 2; y = y_hi * 2 + y_lo), z: 4, core: 2. Of those that a mesh axis runs over, the one named last changes fastest.
Arguments:
- points: bfloat16 [64, 262144], P(None, ('gx', 'gy')), may hold values from -6 to 6
- vectors: bfloat16 [32, 262144], P(None, ('gx', 'gy')), may hold values from -6 to 6
- leaf_pick: int32 [512, 128], P(('gx', 'gy')), may hold values from 0 to 511
- leaf_assign: int32 [512, 512], P(('gx', 'gy')), may hold values from 0 to 127
- device_pick: int32 [128, 128], P(('gx', 'gy')), may hold values from 0 to 511
- device_assign: int32 [128, 512], P(('gx', 'gy')), may hold values from 0 to 127
- node_pick: int32 [16, 7, 128], P('gx'), may hold values from 0 to 255
- node_assign: int32 [16, 7, 256], P('gx'), may hold values from 0 to 127
- far_mask: int32 [16, 16], P('gx'), may hold values from 0 to 1, as said below
- near_lower: int32 [128, 8, 12], P(('gx', 'gy')), may hold values from -1 to 3, as said below
- near_upper: int32 [128, 8, 12], P(('gx', 'gy')), may hold values from 0 to 3, as said below
Outputs:
- potential: float32 [32, 262144], P(None, ('gx', 'gy'))
The draws below stay inside these ranges and needn't reach their ends.
Inputs may be any that keep to these rules, and one draw needn't show every extreme that they name: near_lower[d, o, j] is a local leaf of device d forming a near pair with local leaf near_upper[d, o, j] of device d + o + 1, or -1 for an empty slot; the slots of one d and o never name the same pair of leaves, and no live slot names a device past the last. `near_upper`: A local leaf of device d + o + 1, read only where near_lower is live. `far_mask`: Symmetric, zero on the diagonal, one where the two group indices differ by exactly 1.
All inputs are finite; a program needn't handle non-finite values.
Results may differ from the reference program's by a relative error of at most 0.0015.
Values may be sent and summed in bfloat16 or wider, within the bound.
A program may use at most 128 MiB of HBM per device.

```python
import jax
import jax.numpy as jnp
from jax import lax

DIM = 64
COLS = 32
LEAF = 512
SKEL = 128
LPD = 4
SLOTS = 12
REACH = 8
LEAVES = 512
NPTS = 262144
N_GX = 16
N_GY = 8
DEVICES = 128


def leaf_codes(row_key):
    return jax.random.permutation(row_key, LPD * LPD)[:SLOTS].astype(jnp.int32)


def near_draw(key):
    near_key = jax.random.fold_in(key, 7)
    row_keys = jax.random.split(jax.random.fold_in(near_key, 1), DEVICES * REACH)
    pair_codes = jax.vmap(leaf_codes)(row_keys).reshape(DEVICES, REACH, SLOTS)
    powers = jax.random.randint(jax.random.fold_in(near_key, 2), (DEVICES,), 1, 5)
    weights = jnp.left_shift(jnp.ones_like(powers), powers)
    slot_rolls = jax.random.randint(jax.random.fold_in(near_key, 3), (DEVICES, REACH, SLOTS), 0, 8)
    device_ids = jnp.arange(DEVICES, dtype=jnp.int32)[:, None, None]
    offsets = jnp.arange(1, REACH + 1, dtype=jnp.int32)[None, :, None]
    live_slots = (slot_rolls < weights[:, None, None]) & (device_ids + offsets < DEVICES)
    lower_leaf = jnp.where(live_slots, pair_codes // LPD, -1).astype(jnp.int32)
    upper_leaf = (pair_codes % LPD).astype(jnp.int32)
    return (lower_leaf, upper_leaf)


def draw_near_lower(key, part):
    return near_draw(key)[0]


def draw_near_upper(key, part):
    return near_draw(key)[1]


def draw_far_mask(key, part):
    coin_flips = jax.random.randint(jax.random.fold_in(key, 21), (N_GX, N_GX), 0, 2)
    row_ids = jnp.arange(N_GX, dtype=jnp.int32)[:, None]
    col_ids = jnp.arange(N_GX, dtype=jnp.int32)[None, :]
    symmetric = jnp.where(row_ids < col_ids, coin_flips, coin_flips.T)
    distance = jnp.abs(row_ids - col_ids)
    flagged = jnp.where(distance == 1, 1, symmetric)
    return jnp.where(distance >= 1, flagged, 0).astype(jnp.int32)


def touch_ends(drawn, own_key, smallest, largest):
    shape = drawn.shape
    spot = [jax.random.randint(jax.random.fold_in(own_key, axis), (), 0, shape[axis]) for axis in range(len(shape))]
    drawn = drawn.at[tuple(spot)].set(smallest)
    longest = shape.index(max(shape))
    spot[longest] = (spot[longest] + 1) % shape[longest]
    return drawn.at[tuple(spot)].set(largest)


def level_of(key, extent, cuts, low, largest):
    gain = 1.0
    for dim, parts in cuts:
        heights = jax.random.uniform(jax.random.fold_in(jax.random.fold_in(key, 6), dim), (parts,), jnp.float32, low / len(cuts), largest / len(cuts))
        gain = gain * jnp.repeat(jnp.exp(heights), extent[dim] // parts).reshape((-1,) + (1,) * (len(extent) - 1 - dim))
    return gain


def centred(own_key, shape, width, bound, pieces=(), kind=jnp.bfloat16):
    gain = level_of(own_key, shape, pieces, -0.22, 0.18) if pieces else 1.0
    values = jax.random.normal(own_key, shape, jnp.float32) * width * gain
    return jnp.minimum(jnp.maximum(values, -bound), bound).astype(kind)


def setup_inputs(seed: int = 0) -> dict:
    seeds = jax.random.split(jax.random.key(seed), 12)
    return {
        "points": centred(seeds[0], (DIM, NPTS), 1.0, 6.0, ((1, 128),)),
        "vectors": centred(seeds[1], (COLS, NPTS), 1.0, 6.0, ((1, 128),)),
        "leaf_pick": touch_ends(jax.random.randint(seeds[2], (LEAVES, SKEL), 0, LEAF), jax.random.fold_in(seeds[2], 1), 0, LEAF - 1).astype(jnp.int32),
        "leaf_assign": touch_ends(jax.random.randint(seeds[3], (LEAVES, LEAF), 0, SKEL), jax.random.fold_in(seeds[3], 1), 0, SKEL - 1).astype(jnp.int32),
        "device_pick": touch_ends(jax.random.randint(seeds[4], (DEVICES, SKEL), 0, LPD * SKEL), jax.random.fold_in(seeds[4], 1), 0, (LPD * SKEL) - 1).astype(jnp.int32),
        "device_assign": touch_ends(jax.random.randint(seeds[5], (DEVICES, LPD * SKEL), 0, SKEL), jax.random.fold_in(seeds[5], 1), 0, SKEL - 1).astype(jnp.int32),
        "node_pick": touch_ends(jax.random.randint(seeds[6], (N_GX, N_GY - 1, SKEL), 0, 2 * SKEL), jax.random.fold_in(seeds[6], 1), 0, (2 * SKEL) - 1).astype(jnp.int32),
        "node_assign": touch_ends(jax.random.randint(seeds[7], (N_GX, N_GY - 1, 2 * SKEL), 0, SKEL), jax.random.fold_in(seeds[7], 1), 0, SKEL - 1).astype(jnp.int32),
        "far_mask": draw_far_mask(jax.random.fold_in(seeds[11], 71), 0),
        "near_lower": draw_near_lower(jax.random.fold_in(seeds[11], 71), 0),
        "near_upper": draw_near_upper(jax.random.fold_in(seeds[11], 71), 0),
    }


KERNEL_RATE = 2.0


def kernel_block(source, target):
    decay_rate = KERNEL_RATE / source.shape[0]
    source_wide = source.astype(jnp.float32)
    target_wide = target.astype(jnp.float32)
    source_norm = jnp.sum(source_wide * source_wide, axis=0)
    target_norm = jnp.sum(target_wide * target_wide, axis=0)
    products = lax.dot_general(source, target, (((0,), (0,)), ((), ())), preferred_element_type=jnp.float32)
    return jnp.exp(-decay_rate * (source_norm[:, None] + target_norm[None, :] - 2.0 * products))


def add_columns(running, terms, first_col):
    first_col = jnp.asarray(first_col).astype(jnp.int32)
    current = lax.dynamic_slice_in_dim(running, first_col, terms.shape[1], 1)
    return lax.dynamic_update_slice_in_dim(running, current + terms, first_col, 1)


def pick_columns(table_matrix, col_index):
    return jnp.take(table_matrix, col_index, axis=1)


def sum_skeleton(weights, assignment):
    return jax.ops.segment_sum(weights.T, assignment, num_segments=SKEL).T


def near_field(points, columns, near_lower, near_upper):
    device_cols = LPD * LEAF
    start_terms = jnp.zeros((COLS, points.shape[1]), jnp.float32)

    def per_device(device, running):
        device = jnp.asarray(device).astype(jnp.int32)
        first_col = device * device_cols
        device_points = lax.dynamic_slice_in_dim(points, first_col, device_cols, 1)
        device_values = lax.dynamic_slice_in_dim(columns, first_col, device_cols, 1)

        def per_target(target, inner_terms):
            target_col = jnp.asarray(target).astype(jnp.int32) * LEAF
            target_points = lax.dynamic_slice_in_dim(device_points, target_col, LEAF, 1)
            kernel_tile = kernel_block(device_points, target_points).astype(jnp.bfloat16)
            self_terms = jnp.dot(device_values, kernel_tile, preferred_element_type=jnp.float32)
            return add_columns(inner_terms, self_terms, first_col + target_col)

        running = lax.fori_loop(0, LPD, per_target, running)

        def per_pair(pair_index, inner_terms):
            pair_index = jnp.asarray(pair_index).astype(jnp.int32)
            offset = pair_index // SLOTS
            slot_index = pair_index % SLOTS
            lower_leaf = near_lower[device, offset, slot_index].astype(jnp.int32)
            upper_leaf = near_upper[device, offset, slot_index].astype(jnp.int32)
            live_scale = (lower_leaf >= 0).astype(jnp.float32)
            lower_col = first_col + jnp.maximum(lower_leaf, 0) * LEAF
            upper_col = jnp.minimum((device + offset + 1) * device_cols + upper_leaf * LEAF, points.shape[1] - LEAF)
            low_points = lax.dynamic_slice_in_dim(points, lower_col, LEAF, 1)
            low_values = lax.dynamic_slice_in_dim(columns, lower_col, LEAF, 1)
            high_points = lax.dynamic_slice_in_dim(points, upper_col, LEAF, 1)
            high_values = lax.dynamic_slice_in_dim(columns, upper_col, LEAF, 1)
            kernel_tile = kernel_block(low_points, high_points).astype(jnp.bfloat16)
            to_upper = live_scale * jnp.dot(low_values, kernel_tile, preferred_element_type=jnp.float32)
            to_lower = live_scale * lax.dot_general(high_values, kernel_tile, (((1,), (1,)), ((), ())), preferred_element_type=jnp.float32)
            inner_terms = add_columns(inner_terms, to_lower, lower_col)
            return add_columns(inner_terms, to_upper, upper_col)

        return lax.fori_loop(0, REACH * SLOTS, per_pair, running)

    return lax.fori_loop(0, DEVICES, per_device, start_terms)


def far_field(points, columns, leaf_pick, leaf_assign, device_pick, device_assign, node_pick, node_assign, far_mask):
    leaves = LPD * DEVICES
    leaf_points = points.reshape(DIM, leaves, LEAF)
    leaf_values = columns.reshape(COLS, leaves, LEAF).astype(jnp.float32)
    skeleton_points = jax.vmap(pick_columns, in_axes=(1, 0))(leaf_points, leaf_pick)
    skeleton_weights = jax.vmap(sum_skeleton, in_axes=(1, 0))(leaf_values, leaf_assign)
    joined_points = skeleton_points.reshape(DEVICES, LPD, DIM, SKEL).transpose(0, 2, 1, 3).reshape(DEVICES, DIM, LPD * SKEL)
    joined_weights = skeleton_weights.reshape(DEVICES, LPD, COLS, SKEL).transpose(0, 2, 1, 3).reshape(DEVICES, COLS, LPD * SKEL)
    node_points = jax.vmap(pick_columns)(joined_points, device_pick).reshape(N_GX, N_GY, DIM, SKEL)
    node_weights = jax.vmap(sum_skeleton)(joined_weights, device_assign).reshape(N_GX, N_GY, COLS, SKEL)
    levels = N_GY.bit_length() - 1
    for level_index in range(1, levels + 1):
        node_count = N_GY >> level_index
        pair_points = node_points.reshape(N_GX, node_count, 2, DIM, SKEL).transpose(0, 1, 3, 2, 4).reshape(N_GX * node_count, DIM, 2 * SKEL)
        pair_weights = node_weights.reshape(N_GX, node_count, 2, COLS, SKEL).transpose(0, 1, 3, 2, 4).reshape(N_GX * node_count, COLS, 2 * SKEL)
        picks = node_pick[:, node_count - 1:2 * node_count - 1].reshape(N_GX * node_count, SKEL)
        assignments = node_assign[:, node_count - 1:2 * node_count - 1].reshape(N_GX * node_count, 2 * SKEL)
        node_points = jax.vmap(pick_columns)(pair_points, picks).reshape(N_GX, node_count, DIM, SKEL)
        node_weights = jax.vmap(sum_skeleton)(pair_weights, assignments).reshape(N_GX, node_count, COLS, SKEL)
    root_points = node_points[:, 0]
    root_weights = node_weights[:, 0]

    def kernels_from(source_root):
        return jax.vmap(kernel_block, in_axes=(None, 0))(source_root, root_points)

    root_kernels = jax.vmap(kernels_from)(root_points)
    far_flags = far_mask.astype(jnp.float32)
    root_potential = jnp.einsum("gh,hcs,hgst->gct", far_flags, root_weights, root_kernels, precision=lax.Precision.HIGHEST)
    node_potential = root_potential[:, None]
    for level_index in range(levels, 0, -1):
        node_count = N_GY >> level_index
        assignments = node_assign[:, node_count - 1:2 * node_count - 1].reshape(N_GX * node_count, 2 * SKEL)
        child_potential = jax.vmap(pick_columns)(node_potential.reshape(N_GX * node_count, COLS, SKEL), assignments)
        node_potential = child_potential.reshape(N_GX, node_count, COLS, 2, SKEL).transpose(0, 1, 3, 2, 4).reshape(N_GX, 2 * node_count, COLS, SKEL)
    device_potential = node_potential.reshape(DEVICES, COLS, SKEL)
    leaf_joined = jax.vmap(pick_columns)(device_potential, device_assign)
    leaf_potential = leaf_joined.reshape(DEVICES, COLS, LPD, SKEL).transpose(0, 2, 1, 3).reshape(leaves, COLS, SKEL)
    point_potential = jax.vmap(pick_columns)(leaf_potential, leaf_assign)
    return point_potential.transpose(1, 0, 2).reshape(COLS, leaves * LEAF)


def reference(points, vectors, leaf_pick, leaf_assign, device_pick, device_assign, node_pick, node_assign, far_mask, near_lower, near_upper):
    near_terms = near_field(points, vectors, near_lower, near_upper)
    far_terms = far_field(points, vectors, leaf_pick, leaf_assign, device_pick, device_assign, node_pick, node_assign, far_mask)
    return near_terms + far_terms
```

```python
import jax
import jax.numpy as jnp
from jax import lax
from jax.experimental import pallas as pl
from jax.experimental.pallas import tpu as pltpu
from jax.sharding import PartitionSpec as P

DIM = 64
COLS = 32
LEAF = 512
SKEL = 128
LPD = 4
BLOCK = LPD * LEAF
SLOTS = 12
NGX = 16
NGY = 8
RING = 4
AUG = 128
CHUNK = SKEL // NGY
STRIP = 128
MESH = pl.DeviceIdType.MESH
BF = jnp.bfloat16
F32 = jnp.float32


def nn(a, b, precision=None):
    return lax.dot_general(
        a, b, (((1,), (0,)), ((), ())), preferred_element_type=F32, precision=precision
    )


def nt(a, b):
    return lax.dot_general(a, b, (((1,), (1,)), ((), ())), preferred_element_type=F32)


def three_parts(row):
    high = row.astype(BF).astype(F32)
    rest = row - high
    middle = rest.astype(BF).astype(F32)
    return high, middle, rest - middle


def tail_rows(points, norm_first):
    wide = points.astype(F32)
    parts = three_parts(jnp.sum(wide * wide, axis=0, keepdims=True) * (-1.0 / 32.0))
    row = lax.broadcasted_iota(jnp.int32, (DIM, points.shape[1]), 0)
    at = 0 if norm_first else 3
    ones_at = 3 - at
    tail = jnp.where((row >= ones_at) & (row < ones_at + 3), 1.0, 0.0)
    for k in range(3):
        tail = jnp.where(row == at + k, parts[k], tail)
    return tail.astype(BF)


def build_upper(points, upper_ref, which):
    for leaf in range(LPD):
        cols = pl.ds(leaf * LEAF, LEAF)
        chunk = points[:, cols]
        upper_ref[which, leaf, 0:DIM, :] = chunk
        upper_ref[which, leaf, DIM:AUG, :] = tail_rows(chunk, False)


def build_lower(points, lower_ref):
    for leaf in range(LPD):
        cols = pl.ds(leaf * LEAF, LEAF)
        chunk = points[:, cols]
        both = jnp.concatenate([chunk * BF(1.0 / 16.0), tail_rows(chunk, True)], axis=0)
        lower_ref[leaf] = both.T


def build_leaves(vectors, leaves_ref):
    for leaf in range(LPD):
        leaves_ref[leaf] = vectors[:, leaf * LEAF : (leaf + 1) * LEAF]


def kernel_tile(lower_ref, upper_ref, which, low, high, out_ref):
    upper = upper_ref[which, high]
    for at in range(0, LEAF, STRIP):
        exponent = nn(lower_ref[low, at : at + STRIP, :], upper)
        out_ref[at : at + STRIP, :] = jnp.exp(exponent).astype(BF)


def fused(
    points_ref,
    vectors_ref,
    leaf_pick_ref,
    leaf_assign_ref,
    device_pick_ref,
    device_assign_ref,
    node_pick_ref,
    node_assign_ref,
    far_mask_ref,
    low_s,
    high_s,
    low_v,
    high_v,
    out_ref,
    got_points,
    got_vectors,
    upper_vectors,
    lower_vectors,
    codes_v,
    codes_s,
    lower,
    upper,
    acc_low,
    acc_up,
    send_terms,
    got_terms,
    tile_a,
    tile_b,
    composed,
    share,
    share_got,
    chunk_sum,
    roots,
    targets,
    part,
    part_got,
    near_send,
    near_recv,
    code_send,
    code_recv,
    code_local,
    pass_send,
    pass_recv,
    back_send,
    back_recv,
    share_send,
    share_recv,
    root_send,
    root_recv,
    target_send,
    target_recv,
    part_send,
    part_recv,
):
    gx = lax.axis_index("gx")
    gy = lax.axis_index("gy")
    flat = gx * NGY + gy
    x = gy % RING
    base = gy - x

    def at_flat(step):
        other = lax.rem(flat + step + NGX * NGY, NGX * NGY)
        return (other // NGY, lax.rem(other, NGY))

    def in_ring(step):
        return (gx, base + lax.rem(x + step, RING))

    def mate_gy(step):
        return (gx, lax.rem(gy + step, NGY))

    def mate_gx(step):
        return (lax.rem(gx + step, NGX), gy)

    barrier = pltpu.get_barrier_semaphore()
    greeted = [mate_gy(s) for s in range(1, NGY)] + [mate_gx(s) for s in range(1, NGX)]
    greeted += [at_flat(4), at_flat(-4), at_flat(8), at_flat(-8)]
    for device in greeted:
        pl.semaphore_signal(barrier, inc=1, device_id=device, device_id_type=MESH)
    pl.semaphore_wait(barrier, len(greeted))

    started = []

    def send(src, dst, send_sem, recv_sem, device):
        copy = pltpu.make_async_remote_copy(
            src_ref=src,
            dst_ref=dst,
            send_sem=send_sem,
            recv_sem=recv_sem,
            device_id=device,
            device_id_type=MESH,
        )
        copy.start()
        started.append(copy)
        return copy

    ring_steps = (1, 3, 2)
    code_copies = []
    for k, step in enumerate(ring_steps):
        to = in_ring(RING - step)
        code_copies.append(
            (
                send(low_v, codes_v.at[k, 0], code_send.at[2 * k], code_recv.at[2 * k], to),
                send(high_v, codes_v.at[k, 1], code_send.at[2 * k + 1], code_recv.at[2 * k + 1], to),
            )
        )
    near = [None] * 5

    def send_block(slot, device):
        vector_dst = got_vectors.at[slot]
        near[slot] = (
            send(points_ref, got_points.at[slot], near_send.at[2 * slot], near_recv.at[2 * slot], device),
            send(vectors_ref, vector_dst, near_send.at[2 * slot + 1], near_recv.at[2 * slot + 1], device),
        )

    send_block(1, at_flat(-8))
    send_block(0, at_flat(-4))
    send_block(2, in_ring(3))
    send_block(3, in_ring(1))

    build_leaves(vectors_ref, upper_vectors.at[0])
    build_leaves(vectors_ref, lower_vectors)
    build_upper(points_ref, upper, 0)
    build_lower(points_ref, lower)
    acc_up[...] = jnp.zeros_like(acc_up)
    acc_low[...] = jnp.zeros_like(acc_low)

    heaps = (3 + gy // 2, 1 + gy // 4, 0)
    sides = (gy % 2, (gy // 2) % 2, gy // 4)
    square = lax.broadcasted_iota(jnp.int32, (SKEL, SKEL), 0)

    def hot(condition):
        return jnp.where(condition, 1.0, 0.0).astype(BF)

    path = None
    for level in range(3):
        row = node_assign_ref[
            heaps[level], :, pl.ds(pl.multiple_of(sides[level] * SKEL, SKEL), SKEL)
        ]
        step = hot(square == row)
        path = step if path is None else nn(step, path).astype(BF)
    tall = lax.broadcasted_iota(jnp.int32, (SKEL, LEAF), 0)
    weights = jnp.zeros((SKEL, COLS), F32)
    for leaf in range(LPD):
        cols = slice(leaf * LEAF, (leaf + 1) * LEAF)
        skel = slice(leaf * SKEL, (leaf + 1) * SKEL)
        to_root = nn(path, hot(square == device_assign_ref[:, skel])).astype(BF)
        whole = nn(to_root, hot(tall == leaf_assign_ref[leaf : leaf + 1, :])).astype(BF)
        composed[:, cols] = whole
        weights += nt(whole, vectors_ref[:, cols])
    leaf_rows = lax.broadcasted_iota(jnp.int32, (LEAF, SKEL), 0)
    node_points = jnp.zeros((DIM, SKEL), F32)
    for leaf in range(LPD):
        cols = slice(leaf * LEAF, (leaf + 1) * LEAF)
        picked = nn(points_ref[:, cols], hot(leaf_rows == leaf_pick_ref[leaf : leaf + 1, :]))
        node_points += nn(picked.astype(BF), hot(square + leaf * SKEL == device_pick_ref[...]))
    for level in range(3):
        picks = node_pick_ref[heaps[level]]
        node_points = nn(node_points.astype(BF), hot(square + sides[level] * SKEL == picks))
    share[:, 0:DIM] = jnp.concatenate([node_points, jnp.zeros((SKEL - DIM, SKEL), F32)], axis=0).T[:, 0:DIM]
    share[:, DIM : DIM + COLS] = weights
    share[:, DIM + COLS :] = jnp.zeros((SKEL, SKEL - DIM - COLS), F32)

    def apply_own(tile_ref, low, high):
        low_at = pl.multiple_of(low * LEAF, LEAF)
        high_at = pl.multiple_of(high * LEAF, LEAF)
        tile = tile_ref[...]
        acc_up[0, :, pl.ds(high_at, LEAF)] += nn(upper_vectors[0, low], tile)
        acc_low[0, :, pl.ds(low_at, LEAF)] += nt(upper_vectors[0, high], tile)

    def own_pair(n):
        low = (n >= 3).astype(jnp.int32) + (n >= 5).astype(jnp.int32)
        high = jnp.where(n < 3, n + 1, jnp.where(n < 5, n - 1, 3))
        return low, high

    kernel_tile(lower, upper, 0, 0, 1, tile_a)

    def own_step(m, carry):
        low0, high0 = own_pair(2 * m)
        low1, high1 = own_pair(2 * m + 1)
        low2, high2 = own_pair(jnp.minimum(2 * m + 2, 5))
        kernel_tile(lower, upper, 0, low1, high1, tile_b)
        apply_own(tile_a, low0, high0)
        kernel_tile(lower, upper, 0, low2, high2, tile_a)
        apply_own(tile_b, low1, high1)
        return carry

    lax.fori_loop(0, 3, own_step, 0)

    def own_diagonal(leaf, carry):
        at = pl.multiple_of(leaf * LEAF, LEAF)
        kernel_tile(lower, upper, 0, leaf, leaf, tile_a)
        acc_up[0, :, pl.ds(at, LEAF)] += nn(upper_vectors[0, leaf], tile_a[...])
        return carry

    lax.fori_loop(0, LPD, own_diagonal, 0)

    share_copies = []
    for s in range(1, NGY):
        to = mate_gy(s)
        rows = pl.ds(pl.multiple_of(to[1] * CHUNK, CHUNK), CHUNK)
        share_copies.append(
            send(share.at[rows, :], share_got.at[s - 1], share_send.at[s - 1], share_recv.at[s - 1], to)
        )

    for copy in near[0]:
        copy.wait_recv()
    for copy in near[1]:
        copy.wait_recv()
    build_upper(got_points.at[0], upper, 1)
    build_upper(got_points.at[1], upper, 2)
    build_leaves(got_vectors.at[0], upper_vectors.at[1])
    build_leaves(got_vectors.at[1], upper_vectors.at[2])

    def stage(k, step, low_codes, high_codes):
        i = lax.rem(x + step, RING)
        first = RING + x - i - 1
        other = jnp.where(i < x, x - i - 1, 2 * RING + x - i - 1)
        other_upper = jnp.where(i < x, 0, 2)

        def slot(n):
            far_half = n >= SLOTS
            offset = jnp.where(far_half, other, first)
            which = jnp.where(far_half, other_upper, 1)
            at = n - jnp.where(far_half, SLOTS, 0)
            return low_codes[offset, at], high_codes[offset, at], which

        def make(n, tile_ref):
            low, high, which = slot(n)
            kernel_tile(lower, upper, which, jnp.maximum(low, 0), high, tile_ref)

        def apply(n, tile_ref):
            low, high, which = slot(n)
            tile = tile_ref[...]
            to_upper = nn(lower_vectors[jnp.maximum(low, 0)], tile)
            to_lower = nt(upper_vectors[which, high], tile)
            live = low >= 0
            for leaf in range(LPD):
                cols = slice(leaf * LEAF, (leaf + 1) * LEAF)
                acc_up[which, :, cols] += jnp.where(live & (high == leaf), to_upper, 0.0)
                acc_low[k, :, cols] += jnp.where(low == leaf, to_lower, 0.0)

        make(0, tile_a)

        def pair(m, carry):
            make(2 * m + 1, tile_b)
            apply(2 * m, tile_a)
            make(jnp.minimum(2 * m + 2, 2 * SLOTS - 1), tile_a)
            apply(2 * m + 1, tile_b)
            return carry

        lax.fori_loop(0, SLOTS, pair, 0)

    stage(0, 0, low_s, high_s)

    for copy in share_copies:
        copy.wait_recv()
    mine = pl.ds(pl.multiple_of(gy * CHUNK, CHUNK), CHUNK)
    total = share[mine, :]
    for s in range(NGY - 1):
        total += share_got[s]
    chunk_sum[...] = total
    roots[0] = total
    targets[mine, :] = total

    for slot in (2, 3):
        for copy in near[slot]:
            copy.wait_recv()
    half = BLOCK // 2
    forwards = []
    for part_index, (slot, step, start) in enumerate(((2, 3, 0), (3, 1, half))):
        cols = pl.ds(start, half)
        to = in_ring(step)
        forwards.append(
            send(
                got_points.at[slot, :, cols],
                got_points.at[4, :, cols],
                pass_send.at[2 * part_index],
                pass_recv.at[2 * part_index],
                to,
            )
        )
        forwards.append(
            send(
                got_vectors.at[slot, :, cols],
                got_vectors.at[4, :, cols],
                pass_send.at[2 * part_index + 1],
                pass_recv.at[2 * part_index + 1],
                to,
            )
        )
    root_copies = []
    for s in range(1, NGX):
        root_copies.append(
            send(chunk_sum, roots.at[NGX - s], root_send.at[s - 1], root_recv.at[s - 1], mate_gx(s))
        )
    target_copies = []
    for s in range(1, NGY):
        target_copies.append(
            send(chunk_sum, targets.at[mine, :], target_send.at[s - 1], target_recv.at[s - 1], mate_gy(s))
        )
    for pair in code_copies:
        for copy in pair:
            copy.wait_recv()
    local = []
    for k in range(3):
        for h in range(2):
            copy = pltpu.make_async_copy(codes_v.at[k, h], codes_s.at[k, h], code_local.at[2 * k + h])
            copy.start()
            local.append(copy)
    for copy in local:
        copy.wait()

    def give_back(slot, terms, device):
        send_terms[slot] = terms.astype(BF)
        return send(send_terms.at[slot], got_terms.at[slot], back_send.at[slot], back_recv.at[slot], device)

    returned = []

    def ring_stage(k, step, slot):
        build_lower(got_points.at[slot], lower)
        build_leaves(got_vectors.at[slot], lower_vectors)
        stage(
            k,
            step,
            codes_s.at[slot - 2, 0],
            codes_s.at[slot - 2, 1],
        )

    ring_stage(1, 1, 2)
    returned.append(give_back(2, acc_low[1], in_ring(1)))

    for copy in root_copies:
        copy.wait_recv()
    for copy in target_copies:
        copy.wait_recv()
    sources = roots[...].reshape(NGX * CHUNK, SKEL)
    goals = targets[...]
    source_points = sources[:, 0:DIM]
    goal_points = goals.T[0:DIM, :]
    source_norm = jnp.sum(source_points * source_points, axis=1, keepdims=True)
    goal_norm = jnp.sum(goal_points * goal_points, axis=0, keepdims=True)
    products = nn(source_points.astype(BF), goal_points.astype(BF))
    root_kernel = jnp.exp((-2.0 / DIM) * (source_norm + goal_norm - 2.0 * products))
    source_group = lax.broadcasted_iota(jnp.int32, (NGX * CHUNK, NGX), 0) // CHUNK
    group_id = lax.rem(source_group + gx, NGX)
    listed = lax.broadcasted_iota(jnp.int32, (NGX * CHUNK, NGX), 1) == group_id
    flags = jnp.sum(jnp.where(listed, far_mask_ref[...].astype(F32), 0.0), axis=1, keepdims=True)
    flagged = (sources * flags).T[DIM : DIM + COLS, :]
    part[...] = nn(flagged, root_kernel, lax.Precision.HIGHEST)
    part_copies = []
    for s in range(1, NGY):
        part_copies.append(
            send(part, part_got.at[s - 1], part_send.at[s - 1], part_recv.at[s - 1], mate_gy(s))
        )

    ring_stage(2, 3, 3)
    returned.append(give_back(3, acc_low[2], in_ring(3)))
    for copy in forwards:
        copy.wait_recv()
    ring_stage(3, 2, 4)
    returned.append(give_back(4, acc_low[3], in_ring(2)))
    returned.append(give_back(0, acc_up[1], at_flat(4)))
    returned.append(give_back(1, acc_up[2], at_flat(8)))

    for copy in part_copies:
        copy.wait_recv()
    potential = part[...]
    for s in range(NGY - 1):
        potential += part_got[s]
    parts = [p.astype(BF) for p in three_parts(potential)]
    for leaf in range(LPD):
        cols = slice(leaf * LEAF, (leaf + 1) * LEAF)
        terms = acc_up[0, :, cols] + acc_low[0, :, cols]
        for p in parts:
            terms += nn(p, composed[:, cols])
        acc_up[0, :, cols] = terms

    for copy in returned:
        copy.wait_recv()
    total_terms = acc_up[0]
    for slot in range(5):
        total_terms += got_terms[slot].astype(F32)
    out_ref[...] = total_terms
    for copy in started:
        copy.wait_send()


def on_device(
    points,
    vectors,
    leaf_pick,
    leaf_assign,
    device_pick,
    device_assign,
    node_pick,
    node_assign,
    far_mask,
    near_lower,
    near_upper,
):
    vmem = pl.BlockSpec(memory_space=pltpu.VMEM)
    smem = pl.BlockSpec(memory_space=pltpu.SMEM)
    dma = pltpu.SemaphoreType.DMA
    low, high = near_lower[0], near_upper[0]
    reach = low.shape[0]
    return pl.pallas_call(
        fused,
        out_shape=jax.ShapeDtypeStruct((COLS, BLOCK), F32),
        in_specs=[vmem] * 9 + [smem] * 2 + [vmem] * 2,
        out_specs=vmem,
        scratch_shapes=[
            pltpu.VMEM((5, DIM, BLOCK), BF),
            pltpu.VMEM((5, COLS, BLOCK), BF),
            pltpu.VMEM((3, LPD, COLS, LEAF), BF),
            pltpu.VMEM((LPD, COLS, LEAF), BF),
            pltpu.VMEM((3, 2, reach, SLOTS), jnp.int32),
            pltpu.SMEM((3, 2, reach, SLOTS), jnp.int32),
            pltpu.VMEM((LPD, LEAF, AUG), BF),
            pltpu.VMEM((3, LPD, AUG, LEAF), BF),
            pltpu.VMEM((RING, COLS, BLOCK), F32),
            pltpu.VMEM((3, COLS, BLOCK), F32),
            pltpu.VMEM((5, COLS, BLOCK), BF),
            pltpu.VMEM((5, COLS, BLOCK), BF),
            pltpu.VMEM((LEAF, LEAF), BF),
            pltpu.VMEM((LEAF, LEAF), BF),
            pltpu.VMEM((SKEL, BLOCK), BF),
            pltpu.VMEM((SKEL, SKEL), F32),
            pltpu.VMEM((NGY - 1, CHUNK, SKEL), F32),
            pltpu.VMEM((CHUNK, SKEL), F32),
            pltpu.VMEM((NGX, CHUNK, SKEL), F32),
            pltpu.VMEM((SKEL, SKEL), F32),
            pltpu.VMEM((COLS, SKEL), F32),
            pltpu.VMEM((NGY - 1, COLS, SKEL), F32),
            dma((10,)),
            dma((10,)),
            dma((6,)),
            dma((6,)),
            dma((6,)),
            dma((4,)),
            dma((4,)),
            dma((5,)),
            dma((5,)),
            dma((NGY - 1,)),
            dma((NGY - 1,)),
            dma((NGX - 1,)),
            dma((NGX - 1,)),
            dma((NGY - 1,)),
            dma((NGY - 1,)),
            dma((NGY - 1,)),
            dma((NGY - 1,)),
        ],
        compiler_params=pltpu.CompilerParams(
            collective_id=0, has_side_effects=True, vmem_limit_bytes=56 * 2**20
        ),
        name="treecode",
    )(
        points,
        vectors,
        leaf_pick,
        leaf_assign,
        device_pick,
        device_assign,
        node_pick[0][:, None, :],
        node_assign[0][:, None, :],
        far_mask,
        low,
        high,
        low,
        high,
    )


def solution(mesh):
    placed = (
        P(None, ("gx", "gy")),
        P(None, ("gx", "gy")),
        P(("gx", "gy"), None),
        P(("gx", "gy"), None),
        P(("gx", "gy"), None),
        P(("gx", "gy"), None),
        P("gx", None, None),
        P("gx", None, None),
        P("gx", None),
        P(("gx", "gy"), None, None),
        P(("gx", "gy"), None, None),
    )
    return jax.shard_map(
        on_device, mesh=mesh, in_specs=placed, out_specs=P(None, ("gx", "gy")), check_vma=False
    )
```

```python
import jax
import jax.numpy as jnp
from jax import lax
from jax.experimental import pallas as pl
from jax.experimental.pallas import tpu as pltpu
from jax.sharding import PartitionSpec as P

DIM = 64
COLS = 32
LEAF = 512
SKEL = 128
LPD = 4
BLOCK = LPD * LEAF
SLOTS = 12
NGX = 16
NGY = 8
RING = 4
AUG = 128
CHUNK = SKEL // NGY
STAGES = (0, 1, 2, 3)
HALF = LEAF // 2
UNROLL = 3
MESH = pl.DeviceIdType.MESH
BF = jnp.bfloat16
F32 = jnp.float32


def nn(a, b, precision=None):
    return lax.dot_general(
        a, b, (((1,), (0,)), ((), ())), preferred_element_type=F32, precision=precision
    )


def nt(a, b):
    return lax.dot_general(a, b, (((1,), (1,)), ((), ())), preferred_element_type=F32)


def three_parts(row):
    high = row.astype(BF).astype(F32)
    rest = row - high
    middle = rest.astype(BF).astype(F32)
    return high, middle, rest - middle


def tail_rows(points, norm_first):
    wide = points.astype(F32)
    parts = three_parts(jnp.sum(wide * wide, axis=0, keepdims=True) * (-1.0 / 32.0))
    row = lax.broadcasted_iota(jnp.int32, (DIM, points.shape[1]), 0)
    at = 0 if norm_first else 3
    ones_at = 3 - at
    tail = jnp.where((row >= ones_at) & (row < ones_at + 3), 1.0, 0.0)
    for k in range(3):
        tail = jnp.where(row == at + k, parts[k], tail)
    return tail.astype(BF)


def build_upper(points, upper_ref, which):
    for leaf in range(LPD):
        cols = pl.ds(leaf * LEAF, LEAF)
        chunk = points[:, cols]
        upper_ref[which, leaf, 0:DIM, :] = chunk
        upper_ref[which, leaf, DIM:AUG, :] = tail_rows(chunk, False)


def build_lower(points, lower_ref):
    for leaf in range(LPD):
        cols = pl.ds(leaf * LEAF, LEAF)
        chunk = points[:, cols]
        both = jnp.concatenate([chunk * BF(1.0 / 16.0), tail_rows(chunk, True)], axis=0)
        lower_ref[leaf] = both.T


def build_leaves(vectors, leaves_ref):
    for leaf in range(LPD):
        leaves_ref[leaf] = vectors[:, leaf * LEAF : (leaf + 1) * LEAF]


def tile_rows(lower_rows, upper, out_ref, at):
    out_ref[at : at + HALF, :] = jnp.exp(nn(lower_rows, upper)).astype(BF)


def fused(
    points_hbm,
    vectors_hbm,
    leaf_pick_ref,
    leaf_assign_ref,
    device_pick_ref,
    device_assign_ref,
    node_pick_ref,
    node_assign_ref,
    far_mask_ref,
    low_s,
    high_s,
    low_v,
    high_v,
    out_ref,
    points_ref,
    vectors_ref,
    got_points,
    got_vectors,
    upper_vectors,
    lower_vectors,
    codes_v,
    codes_s,
    lower,
    upper,
    acc_low,
    acc_up,
    send_terms,
    got_terms,
    tile_a,
    tile_b,
    composed,
    share,
    share_got,
    chunk_sum,
    roots,
    targets,
    part,
    part_got,
    near_send,
    near_recv,
    code_send,
    code_recv,
    code_local,
    own_sem,
    pass_send,
    pass_recv,
    back_send,
    back_recv,
    share_send,
    share_recv,
    root_send,
    root_recv,
    target_send,
    target_recv,
    part_send,
    part_recv,
):
    gx = lax.axis_index("gx")
    gy = lax.axis_index("gy")
    flat = gx * NGY + gy
    x = gy % RING
    base = gy - x

    def at_flat(step):
        other = lax.rem(flat + step + NGX * NGY, NGX * NGY)
        return (other // NGY, lax.rem(other, NGY))

    def in_ring(step):
        return (gx, base + lax.rem(x + step, RING))

    def mate_gy(step):
        return (gx, lax.rem(gy + step, NGY))

    def mate_gx(step):
        return (lax.rem(gx + step, NGX), gy)

    barrier = pltpu.get_barrier_semaphore()
    greeted = [mate_gy(s) for s in range(1, NGY)] + [mate_gx(s) for s in range(1, NGX)]
    greeted += [at_flat(4), at_flat(-4), at_flat(8), at_flat(-8)]
    for device in greeted:
        pl.semaphore_signal(barrier, inc=1, device_id=device, device_id_type=MESH)
    own_copies = [
        pltpu.make_async_copy(points_hbm, points_ref, own_sem.at[0]),
        pltpu.make_async_copy(vectors_hbm, vectors_ref, own_sem.at[1]),
    ]
    for copy in own_copies:
        copy.start()
    acc_up[...] = jnp.zeros_like(acc_up)
    acc_low[...] = jnp.zeros_like(acc_low)
    for copy in own_copies:
        copy.wait()
    build_leaves(vectors_ref, upper_vectors.at[0])
    build_leaves(vectors_ref, lower_vectors.at[0])
    build_upper(points_ref, upper, 0)
    build_lower(points_ref, lower.at[0])
    pl.semaphore_wait(barrier, len(greeted))

    started = []

    def send(src, dst, send_sem, recv_sem, device):
        copy = pltpu.make_async_remote_copy(
            src_ref=src,
            dst_ref=dst,
            send_sem=send_sem,
            recv_sem=recv_sem,
            device_id=device,
            device_id_type=MESH,
        )
        copy.start()
        started.append(copy)
        return copy

    code_copies = []
    for k, step in enumerate(STAGES[1:]):
        to = in_ring(RING - step)
        code_copies.append(
            (
                send(low_v, codes_v.at[k, 0], code_send.at[2 * k], code_recv.at[2 * k], to),
                send(high_v, codes_v.at[k, 1], code_send.at[2 * k + 1], code_recv.at[2 * k + 1], to),
            )
        )
    near = [None] * 5

    def send_block(slot, device):
        vector_dst = got_vectors.at[slot]
        near[slot] = (
            send(points_ref, got_points.at[slot], near_send.at[2 * slot], near_recv.at[2 * slot], device),
            send(vectors_ref, vector_dst, near_send.at[2 * slot + 1], near_recv.at[2 * slot + 1], device),
        )

    send_block(1, at_flat(-8))
    send_block(0, at_flat(-4))
    send_block(2, in_ring(3))
    send_block(3, in_ring(1))

    heaps = (3 + gy // 2, 1 + gy // 4, 0)
    sides = (gy % 2, (gy // 2) % 2, gy // 4)
    square = lax.broadcasted_iota(jnp.int32, (SKEL, SKEL), 0)

    def hot(condition):
        return jnp.where(condition, 1.0, 0.0).astype(BF)

    path = None
    for level in range(3):
        row = node_assign_ref[
            heaps[level], :, pl.ds(pl.multiple_of(sides[level] * SKEL, SKEL), SKEL)
        ]
        step = hot(square == row)
        path = step if path is None else nn(step, path).astype(BF)
    tall = lax.broadcasted_iota(jnp.int32, (SKEL, LEAF), 0)
    weights = jnp.zeros((SKEL, COLS), F32)
    for leaf in range(LPD):
        cols = slice(leaf * LEAF, (leaf + 1) * LEAF)
        skel = slice(leaf * SKEL, (leaf + 1) * SKEL)
        to_root = nn(path, hot(square == device_assign_ref[:, skel])).astype(BF)
        whole = nn(to_root, hot(tall == leaf_assign_ref[leaf : leaf + 1, :])).astype(BF)
        composed[:, cols] = whole
        weights += nt(whole, vectors_ref[:, cols])
    leaf_rows = lax.broadcasted_iota(jnp.int32, (LEAF, SKEL), 0)
    node_points = jnp.zeros((DIM, SKEL), F32)
    for leaf in range(LPD):
        cols = slice(leaf * LEAF, (leaf + 1) * LEAF)
        picked = nn(points_ref[:, cols], hot(leaf_rows == leaf_pick_ref[leaf : leaf + 1, :]))
        node_points += nn(picked.astype(BF), hot(square + leaf * SKEL == device_pick_ref[...]))
    for level in range(3):
        picks = node_pick_ref[heaps[level]]
        node_points = nn(node_points.astype(BF), hot(square + sides[level] * SKEL == picks))
    share[:, 0:DIM] = jnp.concatenate([node_points, jnp.zeros((SKEL - DIM, SKEL), F32)], axis=0).T[:, 0:DIM]
    share[:, DIM : DIM + COLS] = weights
    share[:, DIM + COLS :] = jnp.zeros((SKEL, SKEL - DIM - COLS), F32)

    share_copies = []
    for s in range(1, NGY):
        to = mate_gy(s)
        rows = pl.ds(pl.multiple_of(to[1] * CHUNK, CHUNK), CHUNK)
        share_copies.append(
            send(share.at[rows, :], share_got.at[s - 1], share_send.at[s - 1], share_recv.at[s - 1], to)
        )
    mine = pl.ds(pl.multiple_of(gy * CHUNK, CHUNK), CHUNK)
    half = BLOCK // 2

    def masked(ref, index, codes, base_col, terms):
        for leaf in range(LPD):
            cols = slice(leaf * LEAF + base_col, leaf * LEAF + base_col + HALF)
            ref[index, :, cols] += jnp.where(codes == leaf, terms, 0.0)

    class Slot:
        def __init__(self, k, slot_index):
            step = STAGES[k]
            i = lax.rem(x + step, RING)
            first = RING + x - i - 1
            other = jnp.where(i < x, x - i - 1, 2 * RING + x - i - 1)
            if step == 0:
                second_half, half_a, half_b, up_a, up_b = slot_index >= SLOTS, other, first, 2, 1
            else:
                second_half, half_a, half_b = slot_index >= SLOTS, first, other
                up_a, up_b = 1, jnp.where(i < x, 0, 2)
            offset = jnp.where(second_half, half_b, half_a)
            at = slot_index - jnp.where(second_half, SLOTS, 0)
            lows, highs = (low_s, high_s) if step == 0 else (codes_s.at[k - 1, 0], codes_s.at[k - 1, 1])
            self.low, self.high = lows[offset, at], highs[offset, at]
            self.which = jnp.where(second_half, up_b, up_a)
            self.bank = k % 2
            self.k = k

        def rows(self, at):
            return lower[self.bank, jnp.maximum(self.low, 0), at : at + HALF, :], upper[self.which, self.high]

        def left(self):
            return upper_vectors[self.which, self.high], lower_vectors[self.bank, jnp.maximum(self.low, 0)]

        def add_low(self, base_col, terms):
            masked(acc_low, self.k, self.low, base_col, terms)

        def add_high(self, base_col, terms):
            masked(acc_up, self.which, jnp.where(self.low >= 0, self.high, -1), base_col, terms)

    class Own:
        def __init__(self, low, high):
            self.low, self.high = low, high

        def rows(self, at):
            return lower[0, self.low, at : at + HALF, :], upper[0, self.high]

        def left(self):
            return upper_vectors[0, self.high], upper_vectors[0, self.low]

        def add_low(self, base_col, terms):
            at = self.low * LEAF + base_col
            acc_low[0, :, at : at + HALF] += terms

        def add_high(self, base_col, terms):
            at = self.high * LEAF + base_col
            acc_up[0, :, at : at + HALF] += terms

    def make(item, out_ref):
        for at in (0, HALF):
            tile_rows(*item.rows(at), out_ref, at)

    def step_pair(made, made_ref, used, used_ref, both_ways=True):
        high_values, low_values = used.left()
        if both_ways:
            used.add_low(0, nt(high_values, used_ref[0:HALF, :]))
        if made is not None:
            tile_rows(*made.rows(0), made_ref, 0)
        if both_ways:
            used.add_low(HALF, nt(high_values, used_ref[HALF:LEAF, :]))
        used.add_high(0, nn(low_values, used_ref[:, 0:HALF]))
        if made is not None:
            tile_rows(*made.rows(HALF), made_ref, HALF)
        used.add_high(HALF, nn(low_values, used_ref[:, HALF:LEAF]))

    tiles = (tile_a, tile_b)

    def run(items, after):
        for n, item in enumerate(items):
            made = items[n + 1] if n + 1 < len(items) else after
            step_pair(made, tiles[(n + 1) % 2], item, tiles[n % 2])

    def stage_loop(k, first, count):
        width = 2 * UNROLL

        def trip(m, carry):
            at = first + m * width
            run([Slot(k, at + n) for n in range(width)], Slot(k, at + width))
            return carry

        lax.fori_loop(0, count // width, trip, 0)

    def stage_rest(k, first, count, after):
        run([Slot(k, first + n) for n in range(count)], after)

    def give_back(slot, terms, device):
        send_terms[slot] = terms.astype(BF)
        return send(send_terms.at[slot], got_terms.at[slot], back_send.at[slot], back_recv.at[slot], device)

    def land(*slots):
        for slot in slots:
            for copy in near[slot]:
                copy.wait_recv()

    def land_lower(k, slot):
        build_lower(got_points.at[slot], lower.at[k % 2])
        build_leaves(got_vectors.at[slot], lower_vectors.at[k % 2])

    own_pairs = [Own(a, b) for a in range(LPD) for b in range(a + 1, LPD)]
    make(own_pairs[0], tile_a)
    run(own_pairs[:4], own_pairs[4])
    land(1)
    build_upper(got_points.at[1], upper, 2)
    build_leaves(got_vectors.at[1], upper_vectors.at[2])
    run(own_pairs[4:], Slot(0, 0))

    width = 2 * UNROLL
    stage_loop(0, 0, SLOTS - width)
    land(0)
    build_upper(got_points.at[0], upper, 1)
    build_leaves(got_vectors.at[0], upper_vectors.at[1])
    stage_loop(0, SLOTS - width, SLOTS)

    land(2, 3)
    forwards = []
    for part_index, (slot, step, start) in enumerate(((2, 3, 0), (3, 1, half))):
        cols = pl.ds(start, half)
        to = in_ring(step)
        for which, ref in enumerate((got_points, got_vectors)):
            sem = 2 * part_index + which
            forwards.append(
                send(ref.at[slot, :, cols], ref.at[4, :, cols], pass_send.at[sem], pass_recv.at[sem], to)
            )
    for copy in share_copies:
        copy.wait_recv()
    total = share[mine, :]
    for s in range(NGY - 1):
        total += share_got[s]
    chunk_sum[...] = total
    roots[0] = total
    targets[mine, :] = total
    for pair in code_copies:
        for copy in pair:
            copy.wait_recv()
    local = []
    for k in range(3):
        for h in range(2):
            copy = pltpu.make_async_copy(codes_v.at[k, h], codes_s.at[k, h], code_local.at[2 * k + h])
            copy.start()
            local.append(copy)
    for copy in local:
        copy.wait()
    land_lower(1, 2)
    stage_rest(0, 2 * SLOTS - width, width, Slot(1, 0))

    root_copies = []
    for s in range(1, NGX):
        root_copies.append(
            send(chunk_sum, roots.at[NGX - s], root_send.at[s - 1], root_recv.at[s - 1], mate_gx(s))
        )
    target_copies = []
    for s in range(1, NGY):
        target_copies.append(
            send(chunk_sum, targets.at[mine, :], target_send.at[s - 1], target_recv.at[s - 1], mate_gy(s))
        )

    stage_loop(1, 0, 2 * SLOTS - width)
    for copy in forwards:
        copy.wait_recv()
    land_lower(2, 4)
    stage_rest(1, 2 * SLOTS - width, width, Slot(2, 0))
    returned = [give_back(2, acc_low[1], in_ring(1))]

    for copy in root_copies:
        copy.wait_recv()
    for copy in target_copies:
        copy.wait_recv()
    sources = roots[...].reshape(NGX * CHUNK, SKEL)
    source_points = sources[:, 0:DIM]
    goal_points = targets[...].T[0:DIM, :]
    source_norm = jnp.sum(source_points * source_points, axis=1, keepdims=True)
    goal_norm = jnp.sum(goal_points * goal_points, axis=0, keepdims=True)
    products = nn(source_points.astype(BF), goal_points.astype(BF))
    root_kernel = jnp.exp((-2.0 / DIM) * (source_norm + goal_norm - 2.0 * products))
    source_group = lax.broadcasted_iota(jnp.int32, (NGX * CHUNK, NGX), 0) // CHUNK
    group_id = lax.rem(source_group + gx, NGX)
    listed = lax.broadcasted_iota(jnp.int32, (NGX * CHUNK, NGX), 1) == group_id
    flags = jnp.sum(jnp.where(listed, far_mask_ref[...].astype(F32), 0.0), axis=1, keepdims=True)
    flagged = (sources * flags).T[DIM : DIM + COLS, :]
    part[...] = nn(flagged, root_kernel, lax.Precision.HIGHEST)

    stage_loop(2, 0, 2 * SLOTS - width)
    part_copies = []
    for s in range(1, NGY):
        part_copies.append(
            send(part, part_got.at[s - 1], part_send.at[s - 1], part_recv.at[s - 1], mate_gy(s))
        )
    land_lower(3, 3)
    stage_rest(2, 2 * SLOTS - width, width, Slot(3, 0))
    returned.append(give_back(4, acc_low[2], in_ring(2)))

    stage_loop(3, 0, 2 * SLOTS - width)
    returned.append(give_back(0, acc_up[1], at_flat(4)))
    diagonal = [Own(leaf, leaf) for leaf in range(LPD)]
    build_lower(points_ref, lower.at[0])
    stage_rest(3, 2 * SLOTS - width, width, diagonal[0])
    returned.append(give_back(3, acc_low[3], in_ring(3)))
    returned.append(give_back(1, acc_up[2], at_flat(8)))
    for n in range(LPD):
        made = diagonal[n + 1] if n + 1 < LPD else None
        step_pair(made, tiles[(n + 1) % 2], diagonal[n], tiles[n % 2], both_ways=False)

    for copy in part_copies:
        copy.wait_recv()
    potential = part[...]
    for s in range(NGY - 1):
        potential += part_got[s]
    parts = [p.astype(BF) for p in three_parts(potential)]
    for leaf in range(LPD):
        cols = slice(leaf * LEAF, (leaf + 1) * LEAF)
        terms = acc_up[0, :, cols] + acc_low[0, :, cols]
        for p in parts:
            terms += nn(p, composed[:, cols])
        acc_up[0, :, cols] = terms

    for copy in returned:
        copy.wait_recv()
    total_terms = acc_up[0]
    for slot in range(5):
        total_terms += got_terms[slot].astype(F32)
    out_ref[...] = total_terms
    for copy in started:
        copy.wait_send()


def on_device(
    points,
    vectors,
    leaf_pick,
    leaf_assign,
    device_pick,
    device_assign,
    node_pick,
    node_assign,
    far_mask,
    near_lower,
    near_upper,
):
    vmem = pl.BlockSpec(memory_space=pltpu.VMEM)
    smem = pl.BlockSpec(memory_space=pltpu.SMEM)
    dma = pltpu.SemaphoreType.DMA
    low, high = near_lower[0], near_upper[0]
    reach = low.shape[0]
    return pl.pallas_call(
        fused,
        out_shape=jax.ShapeDtypeStruct((COLS, BLOCK), F32),
        in_specs=[pl.BlockSpec(memory_space=pltpu.HBM)] * 2 + [vmem] * 7 + [smem] * 2 + [vmem] * 2,
        out_specs=vmem,
        scratch_shapes=[
            pltpu.VMEM((DIM, BLOCK), BF),
            pltpu.VMEM((COLS, BLOCK), BF),
            pltpu.VMEM((5, DIM, BLOCK), BF),
            pltpu.VMEM((5, COLS, BLOCK), BF),
            pltpu.VMEM((3, LPD, COLS, LEAF), BF),
            pltpu.VMEM((2, LPD, COLS, LEAF), BF),
            pltpu.VMEM((3, 2, reach, SLOTS), jnp.int32),
            pltpu.SMEM((3, 2, reach, SLOTS), jnp.int32),
            pltpu.VMEM((2, LPD, LEAF, AUG), BF),
            pltpu.VMEM((3, LPD, AUG, LEAF), BF),
            pltpu.VMEM((RING, COLS, BLOCK), F32),
            pltpu.VMEM((3, COLS, BLOCK), F32),
            pltpu.VMEM((5, COLS, BLOCK), BF),
            pltpu.VMEM((5, COLS, BLOCK), BF),
            pltpu.VMEM((LEAF, LEAF), BF),
            pltpu.VMEM((LEAF, LEAF), BF),
            pltpu.VMEM((SKEL, BLOCK), BF),
            pltpu.VMEM((SKEL, SKEL), F32),
            pltpu.VMEM((NGY - 1, CHUNK, SKEL), F32),
            pltpu.VMEM((CHUNK, SKEL), F32),
            pltpu.VMEM((NGX, CHUNK, SKEL), F32),
            pltpu.VMEM((SKEL, SKEL), F32),
            pltpu.VMEM((COLS, SKEL), F32),
            pltpu.VMEM((NGY - 1, COLS, SKEL), F32),
            dma((10,)),
            dma((10,)),
            dma((6,)),
            dma((6,)),
            dma((6,)),
            dma((2,)),
            dma((4,)),
            dma((4,)),
            dma((5,)),
            dma((5,)),
            dma((NGY - 1,)),
            dma((NGY - 1,)),
            dma((NGX - 1,)),
            dma((NGX - 1,)),
            dma((NGY - 1,)),
            dma((NGY - 1,)),
            dma((NGY - 1,)),
            dma((NGY - 1,)),
        ],
        compiler_params=pltpu.CompilerParams(
            collective_id=0, has_side_effects=True, vmem_limit_bytes=56 * 2**20
        ),
        name="treecode",
    )(
        points,
        vectors,
        leaf_pick,
        leaf_assign,
        device_pick,
        device_assign,
        node_pick[0][:, None, :],
        node_assign[0][:, None, :],
        far_mask,
        low,
        high,
        low,
        high,
    )


def solution(mesh):
    placed = (
        P(None, ("gx", "gy")),
        P(None, ("gx", "gy")),
        P(("gx", "gy"), None),
        P(("gx", "gy"), None),
        P(("gx", "gy"), None),
        P(("gx", "gy"), None),
        P("gx", None, None),
        P("gx", None, None),
        P("gx", None),
        P(("gx", "gy"), None, None),
        P(("gx", "gy"), None, None),
    )
    return jax.shard_map(
        on_device, mesh=mesh, in_specs=placed, out_specs=P(None, ("gx", "gy")), check_vma=False
    )
```

```python
import jax
import jax.numpy as jnp
from jax import lax
from jax.experimental import pallas as pl
from jax.experimental.pallas import tpu as pltpu
from jax.sharding import PartitionSpec as P

DIM = 64
COLS = 32
LEAF = 512
SKEL = 128
LPD = 4
BLOCK = LPD * LEAF
SLOTS = 12
NGX = 16
NGY = 8
RING = 4
AUG = 128
CHUNK = SKEL // NGY
HALF = LEAF // 2
UNROLL = 3
MESH = pl.DeviceIdType.MESH
BF = jnp.bfloat16
F32 = jnp.float32


def nn(a, b, precision=None):
    return lax.dot_general(
        a, b, (((1,), (0,)), ((), ())), preferred_element_type=F32, precision=precision
    )


def nt(a, b):
    return lax.dot_general(a, b, (((1,), (1,)), ((), ())), preferred_element_type=F32)


def three_parts(row):
    high = row.astype(BF).astype(F32)
    rest = row - high
    middle = rest.astype(BF).astype(F32)
    return high, middle, rest - middle


def tail_rows(points, norm_first):
    wide = points.astype(F32)
    parts = three_parts(jnp.sum(wide * wide, axis=0, keepdims=True) * (-1.0 / 32.0))
    row = lax.broadcasted_iota(jnp.int32, (DIM, points.shape[1]), 0)
    at = 0 if norm_first else 3
    ones_at = 3 - at
    tail = jnp.where((row >= ones_at) & (row < ones_at + 3), 1.0, 0.0)
    for k in range(3):
        tail = jnp.where(row == at + k, parts[k], tail)
    return tail.astype(BF)


def build_upper(points, upper_ref, which):
    for leaf in range(LPD):
        cols = pl.ds(leaf * LEAF, LEAF)
        chunk = points[:, cols]
        upper_ref[which, leaf, 0:DIM, :] = chunk
        upper_ref[which, leaf, DIM:AUG, :] = tail_rows(chunk, False)


def build_lower(points, lower_ref):
    for leaf in range(LPD):
        cols = pl.ds(leaf * LEAF, LEAF)
        chunk = points[:, cols]
        both = jnp.concatenate([chunk * BF(1.0 / 16.0), tail_rows(chunk, True)], axis=0)
        lower_ref[leaf] = both.T


def build_leaves(vectors, leaves_ref):
    for leaf in range(LPD):
        leaves_ref[leaf] = vectors[:, leaf * LEAF : (leaf + 1) * LEAF]


def tile_rows(lower_rows, upper, out_ref, at):
    out_ref[at : at + HALF, :] = jnp.exp(nn(lower_rows, upper)).astype(BF)


def fused(
    points_hbm,
    vectors_hbm,
    leaf_pick_ref,
    leaf_assign_ref,
    device_pick_ref,
    device_assign_ref,
    node_pick_ref,
    node_assign_ref,
    far_mask_ref,
    low_v,
    high_v,
    out_ref,
    points_ref,
    vectors_ref,
    got_points,
    got_vectors,
    upper_vectors,
    lower_vectors,
    codes_v,
    codes_s,
    lower,
    upper,
    acc_low,
    acc_up,
    send_terms,
    got_terms,
    tile_a,
    tile_b,
    composed,
    share,
    share_got,
    chunk_sum,
    roots,
    targets,
    part,
    part_got,
    near_send,
    near_recv,
    code_send,
    code_recv,
    code_local,
    own_sem,
    pass_send,
    pass_recv,
    back_send,
    back_recv,
    share_send,
    share_recv,
    root_send,
    root_recv,
    target_send,
    target_recv,
    part_send,
    part_recv,
):
    gx = lax.axis_index("gx")
    gy = lax.axis_index("gy")
    flat = gx * NGY + gy
    x = gy % RING
    base = gy - x
    near_step = 1 + 2 * (gx % 2)
    steps = (0, near_step, RING - near_step, 2)

    def at_flat(step):
        other = lax.rem(flat + step + NGX * NGY, NGX * NGY)
        return (other // NGY, lax.rem(other, NGY))

    def in_ring(step):
        return (gx, base + lax.rem(x + step, RING))

    def mate_gy(step):
        return (gx, lax.rem(gy + step, NGY))

    def mate_gx(step):
        return (lax.rem(gx + step, NGX), gy)

    barrier = pltpu.get_barrier_semaphore()
    greeted = [mate_gy(s) for s in range(1, NGY)] + [mate_gx(s) for s in range(1, NGX)]
    greeted += [at_flat(4), at_flat(-4), at_flat(8), at_flat(-8)]
    for device in greeted:
        pl.semaphore_signal(barrier, inc=1, device_id=device, device_id_type=MESH)
    own_copies = [
        pltpu.make_async_copy(points_hbm, points_ref, own_sem.at[0]),
        pltpu.make_async_copy(vectors_hbm, vectors_ref, own_sem.at[1]),
        pltpu.make_async_copy(low_v, codes_s.at[0, 0], code_local.at[6]),
        pltpu.make_async_copy(high_v, codes_s.at[0, 1], code_local.at[7]),
    ]
    for copy in own_copies:
        copy.start()
    acc_up[...] = jnp.zeros_like(acc_up)
    acc_low[...] = jnp.zeros_like(acc_low)
    for copy in own_copies:
        copy.wait()
    build_leaves(vectors_ref, upper_vectors.at[0])
    build_leaves(vectors_ref, lower_vectors.at[0])
    build_upper(points_ref, upper, 0)
    build_lower(points_ref, lower.at[0])
    pl.semaphore_wait(barrier, len(greeted))

    started = []

    def send(src, dst, send_sem, recv_sem, device):
        copy = pltpu.make_async_remote_copy(
            src_ref=src,
            dst_ref=dst,
            send_sem=send_sem,
            recv_sem=recv_sem,
            device_id=device,
            device_id_type=MESH,
        )
        copy.start()
        started.append(copy)
        return copy

    code_copies = []
    for k, step in enumerate(steps[1:]):
        to = in_ring(RING - step)
        code_copies.append(
            (
                send(low_v, codes_v.at[k, 0], code_send.at[2 * k], code_recv.at[2 * k], to),
                send(high_v, codes_v.at[k, 1], code_send.at[2 * k + 1], code_recv.at[2 * k + 1], to),
            )
        )
    near = [None] * 5

    def send_block(slot, device):
        vector_dst = got_vectors.at[slot]
        near[slot] = (
            send(points_ref, got_points.at[slot], near_send.at[2 * slot], near_recv.at[2 * slot], device),
            send(vectors_ref, vector_dst, near_send.at[2 * slot + 1], near_recv.at[2 * slot + 1], device),
        )

    send_block(1, at_flat(-8))
    send_block(2, in_ring(RING - near_step))

    heaps = (3 + gy // 2, 1 + gy // 4, 0)
    sides = (gy % 2, (gy // 2) % 2, gy // 4)
    square = lax.broadcasted_iota(jnp.int32, (SKEL, SKEL), 0)

    def hot(condition):
        return jnp.where(condition, 1.0, 0.0).astype(BF)

    path = None
    for level in range(3):
        row = node_assign_ref[
            heaps[level], :, pl.ds(pl.multiple_of(sides[level] * SKEL, SKEL), SKEL)
        ]
        step = hot(square == row)
        path = step if path is None else nn(step, path).astype(BF)
    tall = lax.broadcasted_iota(jnp.int32, (SKEL, LEAF), 0)
    weights = jnp.zeros((SKEL, COLS), F32)
    for leaf in range(LPD):
        cols = slice(leaf * LEAF, (leaf + 1) * LEAF)
        skel = slice(leaf * SKEL, (leaf + 1) * SKEL)
        to_root = nn(path, hot(square == device_assign_ref[:, skel])).astype(BF)
        whole = nn(to_root, hot(tall == leaf_assign_ref[leaf : leaf + 1, :])).astype(BF)
        composed[:, cols] = whole
        weights += nt(whole, vectors_ref[:, cols])
    leaf_rows = lax.broadcasted_iota(jnp.int32, (LEAF, SKEL), 0)
    node_points = jnp.zeros((DIM, SKEL), F32)
    for leaf in range(LPD):
        cols = slice(leaf * LEAF, (leaf + 1) * LEAF)
        picked = nn(points_ref[:, cols], hot(leaf_rows == leaf_pick_ref[leaf : leaf + 1, :]))
        node_points += nn(picked.astype(BF), hot(square + leaf * SKEL == device_pick_ref[...]))
    for level in range(3):
        picks = node_pick_ref[heaps[level]]
        node_points = nn(node_points.astype(BF), hot(square + sides[level] * SKEL == picks))
    share[:, 0:DIM] = jnp.concatenate([node_points, jnp.zeros((SKEL - DIM, SKEL), F32)], axis=0).T[:, 0:DIM]
    share[:, DIM : DIM + COLS] = weights
    share[:, DIM + COLS :] = jnp.zeros((SKEL, SKEL - DIM - COLS), F32)

    share_copies = []
    for s in range(1, NGY):
        to = mate_gy(s)
        rows = pl.ds(pl.multiple_of(to[1] * CHUNK, CHUNK), CHUNK)
        share_copies.append(
            send(share.at[rows, :], share_got.at[s - 1], share_send.at[s - 1], share_recv.at[s - 1], to)
        )
    mine = pl.ds(pl.multiple_of(gy * CHUNK, CHUNK), CHUNK)
    half = BLOCK // 2

    def masked(ref, index, codes, base_col, terms):
        for leaf in range(LPD):
            cols = slice(leaf * LEAF + base_col, leaf * LEAF + base_col + HALF)
            ref[index, :, cols] += jnp.where(codes == leaf, terms, 0.0)

    class Slot:
        def __init__(self, k, step, first_half, at):
            i = lax.rem(x + step, RING)
            first = RING + x - i - 1
            other = jnp.where(i < x, x - i - 1, 2 * RING + x - i - 1)
            offset = jnp.where(first_half, first, other)
            self.low, self.high = codes_s[k, 0, offset, at], codes_s[k, 1, offset, at]
            self.which = jnp.where(first_half, 1, jnp.where(i < x, 0, 2))
            self.k = k

        def rows(self, at):
            return lower[self.k, jnp.maximum(self.low, 0), at : at + HALF, :], upper[self.which, self.high]

        def left(self):
            return upper_vectors[self.which, self.high], lower_vectors[self.k, jnp.maximum(self.low, 0)]

        def add_low(self, base_col, terms):
            masked(acc_low, self.k, self.low, base_col, terms)

        def add_high(self, base_col, terms):
            masked(acc_up, self.which, jnp.where(self.low >= 0, self.high, -1), base_col, terms)

    class Own:
        def __init__(self, low, high):
            self.low, self.high = low, high

        def rows(self, at):
            return lower[0, self.low, at : at + HALF, :], upper[0, self.high]

        def left(self):
            return upper_vectors[0, self.high], upper_vectors[0, self.low]

        def add_low(self, base_col, terms):
            at = self.low * LEAF + base_col
            acc_low[0, :, at : at + HALF] += terms

        def add_high(self, base_col, terms):
            at = self.high * LEAF + base_col
            acc_up[0, :, at : at + HALF] += terms

    def make(item, out_ref):
        for at in (0, HALF):
            tile_rows(*item.rows(at), out_ref, at)

    def step_pair(made, made_ref, used, used_ref, both_ways=True):
        high_values, low_values = used.left()
        if both_ways:
            used.add_low(0, nt(high_values, used_ref[0:HALF, :]))
        if made is not None:
            tile_rows(*made.rows(0), made_ref, 0)
        if both_ways:
            used.add_low(HALF, nt(high_values, used_ref[HALF:LEAF, :]))
        used.add_high(0, nn(low_values, used_ref[:, 0:HALF]))
        if made is not None:
            tile_rows(*made.rows(HALF), made_ref, HALF)
        used.add_high(HALF, nn(low_values, used_ref[:, HALF:LEAF]))

    tiles = (tile_a, tile_b)

    def run(items, after):
        for n, item in enumerate(items):
            made = items[n + 1] if n + 1 < len(items) else after
            step_pair(made, tiles[(n + 1) % 2], item, tiles[n % 2])

    width = 2 * UNROLL

    def stage_loop(slot, count):
        def trip(m, carry):
            at = m * width
            run([slot(at + n) for n in range(width)], slot(at + width))
            return carry

        lax.fori_loop(0, count // width, trip, 0)

    def stage_rest(slot, first, after):
        run([slot(first + n) for n in range(width)], after)

    def give_back(slot, terms, device):
        send_terms[slot] = terms.astype(BF)
        return send(send_terms.at[slot], got_terms.at[slot], back_send.at[slot], back_recv.at[slot], device)

    def land(*slots):
        for slot in slots:
            for copy in near[slot]:
                copy.wait_recv()

    def land_lower(k, slot):
        land(slot)
        build_lower(got_points.at[slot], lower.at[k])
        build_leaves(got_vectors.at[slot], lower_vectors.at[k])

    def other_of(k):
        return lambda n: Slot(k, steps[k], False, n)

    def first_of_three(n):
        k = n // SLOTS
        step = jnp.where(k == 0, 0, jnp.where(k == 1, steps[1], steps[2]))
        return Slot(k, step, True, n - k * SLOTS)

    def last_two(n):
        first_half = n < SLOTS
        return Slot(3, steps[3], first_half, n - jnp.where(first_half, 0, SLOTS))

    own_pairs = [Own(a, b) for a in range(LPD) for b in range(a + 1, LPD)]
    make(own_pairs[0], tile_a)
    run(own_pairs[:4], own_pairs[4])
    for copy in near[2]:
        copy.wait_send()
    send_block(3, in_ring(near_step))
    send_block(0, at_flat(-4))
    land(1)
    build_upper(got_points.at[1], upper, 2)
    build_leaves(got_vectors.at[1], upper_vectors.at[2])
    run(own_pairs[4:], other_of(0)(0))

    stage_loop(other_of(0), width)
    for pair in code_copies:
        for copy in pair:
            copy.wait_recv()
    local = []
    for k in range(3):
        for h in range(2):
            copy = pltpu.make_async_copy(codes_v.at[k, h], codes_s.at[k + 1, h], code_local.at[2 * k + h])
            copy.start()
            local.append(copy)
    for copy in local:
        copy.wait()
    land_lower(1, 2)
    stage_rest(other_of(0), width, other_of(1)(0))

    stage_loop(other_of(1), width)
    land_lower(2, 3)
    forwards = []
    for part_index, slot in enumerate((2, 3)):
        cols = pl.ds(part_index * half, half)
        to = in_ring(RING - steps[1 + part_index])
        for which, ref in enumerate((got_points, got_vectors)):
            sem = 2 * part_index + which
            forwards.append(
                send(ref.at[slot, :, cols], ref.at[4, :, cols], pass_send.at[sem], pass_recv.at[sem], to)
            )
    near[4] = forwards
    for copy in share_copies:
        copy.wait_recv()
    total = share[mine, :]
    for s in range(NGY - 1):
        total += share_got[s]
    chunk_sum[...] = total
    roots[0] = total
    targets[mine, :] = total
    stage_rest(other_of(1), width, other_of(2)(0))

    root_copies = []
    for s in range(1, NGX):
        root_copies.append(
            send(chunk_sum, roots.at[NGX - s], root_send.at[s - 1], root_recv.at[s - 1], mate_gx(s))
        )
    target_copies = []
    for s in range(1, NGY):
        target_copies.append(
            send(chunk_sum, targets.at[mine, :], target_send.at[s - 1], target_recv.at[s - 1], mate_gy(s))
        )
    stage_loop(other_of(2), width)
    land(0)
    build_upper(got_points.at[0], upper, 1)
    build_leaves(got_vectors.at[0], upper_vectors.at[1])
    stage_rest(other_of(2), width, first_of_three(0))

    stage_loop(first_of_three, 3 * SLOTS - width)
    land_lower(3, 4)
    for copy in root_copies:
        copy.wait_recv()
    for copy in target_copies:
        copy.wait_recv()
    sources = roots[...].reshape(NGX * CHUNK, SKEL)
    source_points = sources[:, 0:DIM]
    goal_points = targets[...].T[0:DIM, :]
    source_norm = jnp.sum(source_points * source_points, axis=1, keepdims=True)
    goal_norm = jnp.sum(goal_points * goal_points, axis=0, keepdims=True)
    products = nn(source_points.astype(BF), goal_points.astype(BF))
    root_kernel = jnp.exp((-2.0 / DIM) * (source_norm + goal_norm - 2.0 * products))
    source_group = lax.broadcasted_iota(jnp.int32, (NGX * CHUNK, NGX), 0) // CHUNK
    group_id = lax.rem(source_group + gx, NGX)
    listed = lax.broadcasted_iota(jnp.int32, (NGX * CHUNK, NGX), 1) == group_id
    flags = jnp.sum(jnp.where(listed, far_mask_ref[...].astype(F32), 0.0), axis=1, keepdims=True)
    flagged = (sources * flags).T[DIM : DIM + COLS, :]
    part[...] = nn(flagged, root_kernel, lax.Precision.HIGHEST)
    stage_rest(first_of_three, 3 * SLOTS - width, last_two(0))
    part_copies = []
    for s in range(1, NGY):
        part_copies.append(
            send(part, part_got.at[s - 1], part_send.at[s - 1], part_recv.at[s - 1], mate_gy(s))
        )
    returned = [give_back(2, acc_low[1], in_ring(steps[1])), give_back(3, acc_low[2], in_ring(steps[2]))]

    stage_loop(last_two, 2 * SLOTS - width)
    returned.append(give_back(0, acc_up[1], at_flat(4)))
    diagonal = [Own(leaf, leaf) for leaf in range(LPD)]
    stage_rest(last_two, 2 * SLOTS - width, diagonal[0])
    returned.append(give_back(4, acc_low[3], in_ring(2)))
    returned.append(give_back(1, acc_up[2], at_flat(8)))
    for n in range(LPD):
        made = diagonal[n + 1] if n + 1 < LPD else None
        step_pair(made, tiles[(n + 1) % 2], diagonal[n], tiles[n % 2], both_ways=False)

    for copy in part_copies:
        copy.wait_recv()
    potential = part[...]
    for s in range(NGY - 1):
        potential += part_got[s]
    parts = [p.astype(BF) for p in three_parts(potential)]
    for leaf in range(LPD):
        cols = slice(leaf * LEAF, (leaf + 1) * LEAF)
        terms = acc_up[0, :, cols] + acc_low[0, :, cols]
        for p in parts:
            terms += nn(p, composed[:, cols])
        acc_up[0, :, cols] = terms

    for copy in returned:
        copy.wait_recv()
    total_terms = acc_up[0]
    for slot in range(5):
        total_terms += got_terms[slot].astype(F32)
    out_ref[...] = total_terms
    for copy in started:
        if not any(copy is done for done in near[2]):
            copy.wait_send()


def on_device(
    points,
    vectors,
    leaf_pick,
    leaf_assign,
    device_pick,
    device_assign,
    node_pick,
    node_assign,
    far_mask,
    near_lower,
    near_upper,
):
    vmem = pl.BlockSpec(memory_space=pltpu.VMEM)
    dma = pltpu.SemaphoreType.DMA
    low, high = near_lower[0], near_upper[0]
    reach = low.shape[0]
    return pl.pallas_call(
        fused,
        out_shape=jax.ShapeDtypeStruct((COLS, BLOCK), F32),
        in_specs=[pl.BlockSpec(memory_space=pltpu.HBM)] * 2 + [vmem] * 9,
        out_specs=vmem,
        scratch_shapes=[
            pltpu.VMEM((DIM, BLOCK), BF),
            pltpu.VMEM((COLS, BLOCK), BF),
            pltpu.VMEM((5, DIM, BLOCK), BF),
            pltpu.VMEM((5, COLS, BLOCK), BF),
            pltpu.VMEM((3, LPD, COLS, LEAF), BF),
            pltpu.VMEM((RING, LPD, COLS, LEAF), BF),
            pltpu.VMEM((3, 2, reach, SLOTS), jnp.int32),
            pltpu.SMEM((RING, 2, reach, SLOTS), jnp.int32),
            pltpu.VMEM((RING, LPD, LEAF, AUG), BF),
            pltpu.VMEM((3, LPD, AUG, LEAF), BF),
            pltpu.VMEM((RING, COLS, BLOCK), F32),
            pltpu.VMEM((3, COLS, BLOCK), F32),
            pltpu.VMEM((5, COLS, BLOCK), BF),
            pltpu.VMEM((5, COLS, BLOCK), BF),
            pltpu.VMEM((LEAF, LEAF), BF),
            pltpu.VMEM((LEAF, LEAF), BF),
            pltpu.VMEM((SKEL, BLOCK), BF),
            pltpu.VMEM((SKEL, SKEL), F32),
            pltpu.VMEM((NGY - 1, CHUNK, SKEL), F32),
            pltpu.VMEM((CHUNK, SKEL), F32),
            pltpu.VMEM((NGX, CHUNK, SKEL), F32),
            pltpu.VMEM((SKEL, SKEL), F32),
            pltpu.VMEM((COLS, SKEL), F32),
            pltpu.VMEM((NGY - 1, COLS, SKEL), F32),
            dma((10,)),
            dma((10,)),
            dma((6,)),
            dma((6,)),
            dma((8,)),
            dma((2,)),
            dma((4,)),
            dma((4,)),
            dma((5,)),
            dma((5,)),
            dma((NGY - 1,)),
            dma((NGY - 1,)),
            dma((NGX - 1,)),
            dma((NGX - 1,)),
            dma((NGY - 1,)),
            dma((NGY - 1,)),
            dma((NGY - 1,)),
            dma((NGY - 1,)),
        ],
        compiler_params=pltpu.CompilerParams(
            collective_id=0, has_side_effects=True, vmem_limit_bytes=56 * 2**20
        ),
        name="treecode",
    )(
        points,
        vectors,
        leaf_pick,
        leaf_assign,
        device_pick,
        device_assign,
        node_pick[0][:, None, :],
        node_assign[0][:, None, :],
        far_mask,
        low,
        high,
    )


def solution(mesh):
    placed = (
        P(None, ("gx", "gy")),
        P(None, ("gx", "gy")),
        P(("gx", "gy"), None),
        P(("gx", "gy"), None),
        P(("gx", "gy"), None),
        P(("gx", "gy"), None),
        P("gx", None, None),
        P("gx", None, None),
        P("gx", None),
        P(("gx", "gy"), None, None),
        P(("gx", "gy"), None, None),
    )
    return jax.shard_map(
        on_device, mesh=mesh, in_specs=placed, out_specs=P(None, ("gx", "gy")), check_vma=False
    )
```

```python
import jax
import jax.numpy as jnp
from jax import lax
from jax.experimental import pallas as pl
from jax.experimental.pallas import tpu as pltpu
from jax.sharding import PartitionSpec as P

DIM = 64
COLS = 32
LEAF = 512
SKEL = 128
LPD = 4
BLOCK = LPD * LEAF
SLOTS = 12
NGX = 16
NGY = 8
RING = 4
AUG = 128
CHUNK = SKEL // NGY
HALF = LEAF // 2
UNROLL = 3
MESH = pl.DeviceIdType.MESH
BF = jnp.bfloat16
F32 = jnp.float32


def nn(a, b, precision=None):
    return lax.dot_general(
        a, b, (((1,), (0,)), ((), ())), preferred_element_type=F32, precision=precision
    )


def nt(a, b):
    return lax.dot_general(a, b, (((1,), (1,)), ((), ())), preferred_element_type=F32)


def three_parts(row):
    high = row.astype(BF).astype(F32)
    rest = row - high
    middle = rest.astype(BF).astype(F32)
    return high, middle, rest - middle


def tail_rows(points, norm_first):
    wide = points.astype(F32)
    parts = three_parts(jnp.sum(wide * wide, axis=0, keepdims=True) * (-1.0 / 32.0))
    row = lax.broadcasted_iota(jnp.int32, (DIM, points.shape[1]), 0)
    at = 0 if norm_first else 3
    ones_at = 3 - at
    tail = jnp.where((row >= ones_at) & (row < ones_at + 3), 1.0, 0.0)
    for k in range(3):
        tail = jnp.where(row == at + k, parts[k], tail)
    return tail.astype(BF)


def build_upper(points, upper_ref, which):
    for leaf in range(LPD):
        cols = pl.ds(leaf * LEAF, LEAF)
        chunk = points[:, cols]
        upper_ref[which, leaf, 0:DIM, :] = chunk
        upper_ref[which, leaf, DIM:AUG, :] = tail_rows(chunk, False)


def build_lower(points, lower_ref):
    for leaf in range(LPD):
        cols = pl.ds(leaf * LEAF, LEAF)
        chunk = points[:, cols]
        both = jnp.concatenate([chunk * BF(1.0 / 16.0), tail_rows(chunk, True)], axis=0)
        lower_ref[leaf] = both.T


def build_leaves(vectors, leaves_ref):
    for leaf in range(LPD):
        leaves_ref[leaf] = vectors[:, leaf * LEAF : (leaf + 1) * LEAF]


def tile_rows(lower_rows, upper, out_ref, at):
    out_ref[at : at + HALF, :] = jnp.exp(nn(lower_rows, upper)).astype(BF)


def fused(
    points_hbm,
    vectors_hbm,
    leaf_pick_ref,
    leaf_assign_ref,
    device_pick_ref,
    device_assign_ref,
    node_pick_ref,
    node_assign_ref,
    far_mask_ref,
    low_v,
    high_v,
    out_ref,
    points_ref,
    vectors_ref,
    got_points,
    got_vectors,
    upper_vectors,
    lower_vectors,
    codes_v,
    codes_s,
    lower,
    upper,
    acc_low,
    acc_up,
    send_terms,
    got_terms,
    tile_a,
    tile_b,
    composed,
    share,
    share_got,
    chunk_sum,
    roots,
    targets,
    part,
    part_got,
    near_send,
    near_recv,
    code_send,
    code_recv,
    code_local,
    own_sem,
    pass_send,
    pass_recv,
    back_send,
    back_recv,
    share_send,
    share_recv,
    root_send,
    root_recv,
    target_send,
    target_recv,
    part_send,
    part_recv,
):
    gx = lax.axis_index("gx")
    gy = lax.axis_index("gy")
    flat = gx * NGY + gy
    x = gy % RING
    base = gy - x
    near_step = 1 + 2 * (gx % 2)
    steps = (0, near_step, RING - near_step, 2)

    def at_flat(step):
        other = lax.rem(flat + step + NGX * NGY, NGX * NGY)
        return (other // NGY, lax.rem(other, NGY))

    def in_ring(step):
        return (gx, base + lax.rem(x + step, RING))

    def mate_gy(step):
        return (gx, lax.rem(gy + step, NGY))

    def mate_gx(step):
        return (lax.rem(gx + step, NGX), gy)

    barrier = pltpu.get_barrier_semaphore()
    greeted = [mate_gy(s) for s in range(1, NGY)] + [mate_gx(s) for s in range(1, NGX)]
    greeted += [at_flat(4), at_flat(-4), at_flat(8), at_flat(-8)]
    for device in greeted:
        pl.semaphore_signal(barrier, inc=1, device_id=device, device_id_type=MESH)
    own_copies = [
        pltpu.make_async_copy(points_hbm, points_ref, own_sem.at[0]),
        pltpu.make_async_copy(vectors_hbm, vectors_ref, own_sem.at[1]),
        pltpu.make_async_copy(low_v, codes_s.at[0, 0], code_local.at[6]),
        pltpu.make_async_copy(high_v, codes_s.at[0, 1], code_local.at[7]),
    ]
    for copy in own_copies:
        copy.start()
    acc_up[...] = jnp.zeros_like(acc_up)
    acc_low[...] = jnp.zeros_like(acc_low)
    for copy in own_copies:
        copy.wait()
    build_leaves(vectors_ref, upper_vectors.at[0])
    build_leaves(vectors_ref, lower_vectors.at[0])
    build_upper(points_ref, upper, 0)
    build_lower(points_ref, lower.at[0])
    pl.semaphore_wait(barrier, len(greeted))

    started = []

    def send(src, dst, send_sem, recv_sem, device):
        copy = pltpu.make_async_remote_copy(
            src_ref=src,
            dst_ref=dst,
            send_sem=send_sem,
            recv_sem=recv_sem,
            device_id=device,
            device_id_type=MESH,
        )
        copy.start()
        started.append(copy)
        return copy

    code_copies = []
    for k, step in enumerate(steps[1:]):
        to = in_ring(RING - step)
        code_copies.append(
            (
                send(low_v, codes_v.at[k, 0], code_send.at[2 * k], code_recv.at[2 * k], to),
                send(high_v, codes_v.at[k, 1], code_send.at[2 * k + 1], code_recv.at[2 * k + 1], to),
            )
        )
    near = [None] * 5

    def send_block(slot, device):
        vector_dst = got_vectors.at[slot]
        near[slot] = (
            send(points_ref, got_points.at[slot], near_send.at[2 * slot], near_recv.at[2 * slot], device),
            send(vectors_ref, vector_dst, near_send.at[2 * slot + 1], near_recv.at[2 * slot + 1], device),
        )

    send_block(1, at_flat(-8))
    send_block(2, in_ring(RING - near_step))

    heaps = (3 + gy // 2, 1 + gy // 4, 0)
    sides = (gy % 2, (gy // 2) % 2, gy // 4)
    square = lax.broadcasted_iota(jnp.int32, (SKEL, SKEL), 0)

    def hot(condition):
        return jnp.where(condition, 1.0, 0.0).astype(BF)

    path = None
    for level in range(3):
        row = node_assign_ref[
            heaps[level], :, pl.ds(pl.multiple_of(sides[level] * SKEL, SKEL), SKEL)
        ]
        step = hot(square == row)
        path = step if path is None else nn(step, path).astype(BF)
    tall = lax.broadcasted_iota(jnp.int32, (SKEL, LEAF), 0)
    weights = jnp.zeros((SKEL, COLS), F32)
    for leaf in range(LPD):
        cols = slice(leaf * LEAF, (leaf + 1) * LEAF)
        skel = slice(leaf * SKEL, (leaf + 1) * SKEL)
        to_root = nn(path, hot(square == device_assign_ref[:, skel])).astype(BF)
        whole = nn(to_root, hot(tall == leaf_assign_ref[leaf : leaf + 1, :])).astype(BF)
        composed[:, cols] = whole
        weights += nt(whole, vectors_ref[:, cols])
    leaf_rows = lax.broadcasted_iota(jnp.int32, (LEAF, SKEL), 0)
    node_points = jnp.zeros((DIM, SKEL), F32)
    for leaf in range(LPD):
        cols = slice(leaf * LEAF, (leaf + 1) * LEAF)
        picked = nn(points_ref[:, cols], hot(leaf_rows == leaf_pick_ref[leaf : leaf + 1, :]))
        node_points += nn(picked.astype(BF), hot(square + leaf * SKEL == device_pick_ref[...]))
    for level in range(3):
        picks = node_pick_ref[heaps[level]]
        node_points = nn(node_points.astype(BF), hot(square + sides[level] * SKEL == picks))
    share[:, 0:DIM] = jnp.concatenate([node_points, jnp.zeros((SKEL - DIM, SKEL), F32)], axis=0).T[:, 0:DIM]
    share[:, DIM : DIM + COLS] = weights
    share[:, DIM + COLS :] = jnp.zeros((SKEL, SKEL - DIM - COLS), F32)

    share_copies = []
    for s in range(1, NGY):
        to = mate_gy(s)
        rows = pl.ds(pl.multiple_of(to[1] * CHUNK, CHUNK), CHUNK)
        share_copies.append(
            send(share.at[rows, :], share_got.at[s - 1], share_send.at[s - 1], share_recv.at[s - 1], to)
        )
    mine = pl.ds(pl.multiple_of(gy * CHUNK, CHUNK), CHUNK)
    half = BLOCK // 2

    def masked(ref, index, codes, base_col, terms):
        for leaf in range(LPD):
            cols = slice(leaf * LEAF + base_col, leaf * LEAF + base_col + HALF)
            ref[index, :, cols] += jnp.where(codes == leaf, terms, 0.0)

    class Slot:
        def __init__(self, k, step, first_half, at):
            i = lax.rem(x + step, RING)
            first = RING + x - i - 1
            other = jnp.where(i < x, x - i - 1, 2 * RING + x - i - 1)
            offset = jnp.where(first_half, first, other)
            self.low, self.high = codes_s[k, 0, offset, at], codes_s[k, 1, offset, at]
            self.which = jnp.where(first_half, 1, jnp.where(i < x, 0, 2))
            self.k = k

        def rows(self, at):
            return lower[self.k, jnp.maximum(self.low, 0), at : at + HALF, :], upper[self.which, self.high]

        def left(self):
            return upper_vectors[self.which, self.high], lower_vectors[self.k, jnp.maximum(self.low, 0)]

        def add_low(self, base_col, terms):
            masked(acc_low, self.k, self.low, base_col, terms)

        def add_high(self, base_col, terms):
            masked(acc_up, self.which, jnp.where(self.low >= 0, self.high, -1), base_col, terms)

    class Own:
        def __init__(self, low, high):
            self.low, self.high = low, high

        def rows(self, at):
            return lower[0, self.low, at : at + HALF, :], upper[0, self.high]

        def left(self):
            return upper_vectors[0, self.high], upper_vectors[0, self.low]

        def add_low(self, base_col, terms):
            at = self.low * LEAF + base_col
            acc_low[0, :, at : at + HALF] += terms

        def add_high(self, base_col, terms):
            at = self.high * LEAF + base_col
            acc_up[0, :, at : at + HALF] += terms

    def make(item, out_ref):
        for at in (0, HALF):
            tile_rows(*item.rows(at), out_ref, at)

    def step_pair(made, made_ref, used, used_ref, both_ways=True):
        high_values, low_values = used.left()
        if both_ways:
            used.add_low(0, nt(high_values, used_ref[0:HALF, :]))
        if made is not None:
            tile_rows(*made.rows(0), made_ref, 0)
        if both_ways:
            used.add_low(HALF, nt(high_values, used_ref[HALF:LEAF, :]))
        used.add_high(0, nn(low_values, used_ref[:, 0:HALF]))
        if made is not None:
            tile_rows(*made.rows(HALF), made_ref, HALF)
        used.add_high(HALF, nn(low_values, used_ref[:, HALF:LEAF]))

    tiles = (tile_a, tile_b)

    def run(items, after, before_last=None):
        for n, item in enumerate(items):
            if before_last is not None and n + 1 == len(items):
                before_last()
            made = items[n + 1] if n + 1 < len(items) else after
            step_pair(made, tiles[(n + 1) % 2], item, tiles[n % 2])

    width = 2 * UNROLL

    def stage_loop(slot, count):
        def trip(m, carry):
            at = m * width
            run([slot(at + n) for n in range(width)], slot(at + width))
            return carry

        lax.fori_loop(0, count // width, trip, 0)

    def stage_rest(slot, first, after, before_last=None):
        run([slot(first + n) for n in range(width)], after, before_last)

    def give_back(slot, terms, device):
        send_terms[slot] = terms.astype(BF)
        return send(send_terms.at[slot], got_terms.at[slot], back_send.at[slot], back_recv.at[slot], device)

    def land(*slots):
        for slot in slots:
            for copy in near[slot]:
                copy.wait_recv()

    def land_lower(k, slot):
        land(slot)
        build_lower(got_points.at[slot], lower.at[k])
        build_leaves(got_vectors.at[slot], lower_vectors.at[k])

    def other_of(k):
        return lambda n: Slot(k, steps[k], False, n)

    def first_of_three(n):
        k = n // SLOTS
        step = jnp.where(k == 0, 0, jnp.where(k == 1, steps[1], steps[2]))
        return Slot(k, step, True, n - k * SLOTS)

    def last_two(n):
        first_half = n < SLOTS
        return Slot(3, steps[3], first_half, n - jnp.where(first_half, 0, SLOTS))

    own_pairs = [Own(a, b) for a in range(LPD) for b in range(a + 1, LPD)]
    make(own_pairs[0], tile_a)
    run(own_pairs[:4], own_pairs[4])
    for copy in near[2]:
        copy.wait_send()
    send_block(3, in_ring(near_step))
    send_block(0, at_flat(-4))

    def land_upper(slot, which):
        land(slot)
        build_upper(got_points.at[slot], upper, which)
        build_leaves(got_vectors.at[slot], upper_vectors.at[which])

    run(own_pairs[4:], other_of(0)(0), lambda: land_upper(1, 2))

    stage_loop(other_of(0), width)
    for pair in code_copies:
        for copy in pair:
            copy.wait_recv()
    local = []
    for k in range(3):
        for h in range(2):
            copy = pltpu.make_async_copy(codes_v.at[k, h], codes_s.at[k + 1, h], code_local.at[2 * k + h])
            copy.start()
            local.append(copy)
    for copy in local:
        copy.wait()
    land_lower(1, 2)
    stage_rest(other_of(0), width, other_of(1)(0))

    stage_loop(other_of(1), width)
    land_lower(2, 3)
    forwards = []
    for part_index, slot in enumerate((2, 3)):
        cols = pl.ds(part_index * half, half)
        to = in_ring(RING - steps[1 + part_index])
        for which, ref in enumerate((got_points, got_vectors)):
            sem = 2 * part_index + which
            forwards.append(
                send(ref.at[slot, :, cols], ref.at[4, :, cols], pass_send.at[sem], pass_recv.at[sem], to)
            )
    near[4] = forwards
    for copy in share_copies:
        copy.wait_recv()
    total = share[mine, :]
    for s in range(NGY - 1):
        total += share_got[s]
    chunk_sum[...] = total
    roots[0] = total
    targets[mine, :] = total
    stage_rest(other_of(1), width, first_of_three(0), lambda: land_upper(0, 1))

    root_copies = []
    for s in range(1, NGX):
        root_copies.append(
            send(chunk_sum, roots.at[NGX - s], root_send.at[s - 1], root_recv.at[s - 1], mate_gx(s))
        )
    target_copies = []
    for s in range(1, NGY):
        target_copies.append(
            send(chunk_sum, targets.at[mine, :], target_send.at[s - 1], target_recv.at[s - 1], mate_gy(s))
        )

    stage_loop(first_of_three, 3 * SLOTS - width)
    land_lower(3, 4)
    for copy in root_copies:
        copy.wait_recv()
    for copy in target_copies:
        copy.wait_recv()
    sources = roots[...].reshape(NGX * CHUNK, SKEL)
    source_points = sources[:, 0:DIM]
    goal_points = targets[...].T[0:DIM, :]
    source_norm = jnp.sum(source_points * source_points, axis=1, keepdims=True)
    goal_norm = jnp.sum(goal_points * goal_points, axis=0, keepdims=True)
    products = nn(source_points.astype(BF), goal_points.astype(BF))
    root_kernel = jnp.exp((-2.0 / DIM) * (source_norm + goal_norm - 2.0 * products))
    source_group = lax.broadcasted_iota(jnp.int32, (NGX * CHUNK, NGX), 0) // CHUNK
    group_id = lax.rem(source_group + gx, NGX)
    listed = lax.broadcasted_iota(jnp.int32, (NGX * CHUNK, NGX), 1) == group_id
    flags = jnp.sum(jnp.where(listed, far_mask_ref[...].astype(F32), 0.0), axis=1, keepdims=True)
    flagged = (sources * flags).T[DIM : DIM + COLS, :]
    part[...] = nn(flagged, root_kernel, lax.Precision.HIGHEST)
    stage_rest(first_of_three, 3 * SLOTS - width, last_two(0))
    part_copies = []
    for s in range(1, NGY):
        part_copies.append(
            send(part, part_got.at[s - 1], part_send.at[s - 1], part_recv.at[s - 1], mate_gy(s))
        )
    returned = [give_back(2, acc_low[1], in_ring(steps[1]))]

    stage_loop(last_two, 2 * SLOTS - width)
    returned.append(give_back(0, acc_up[1], at_flat(4)))
    diagonal = [Own(leaf, leaf) for leaf in range(LPD)]
    stage_rest(last_two, 2 * SLOTS - width, other_of(2)(0))
    returned.append(give_back(4, acc_low[3], in_ring(2)))
    stage_loop(other_of(2), width)
    stage_rest(other_of(2), width, diagonal[0])
    returned.append(give_back(3, acc_low[2], in_ring(steps[2])))
    returned.append(give_back(1, acc_up[2], at_flat(8)))
    for n in range(LPD):
        made = diagonal[n + 1] if n + 1 < LPD else None
        step_pair(made, tiles[(n + 1) % 2], diagonal[n], tiles[n % 2], both_ways=False)

    for copy in part_copies:
        copy.wait_recv()
    potential = part[...]
    for s in range(NGY - 1):
        potential += part_got[s]
    parts = [p.astype(BF) for p in three_parts(potential)]
    for leaf in range(LPD):
        cols = slice(leaf * LEAF, (leaf + 1) * LEAF)
        terms = acc_up[0, :, cols] + acc_low[0, :, cols]
        for p in parts:
            terms += nn(p, composed[:, cols])
        acc_up[0, :, cols] = terms

    for copy in returned:
        copy.wait_recv()
    total_terms = acc_up[0]
    for slot in range(5):
        total_terms += got_terms[slot].astype(F32)
    out_ref[...] = total_terms
    for copy in started:
        if not any(copy is done for done in near[2]):
            copy.wait_send()


def on_device(
    points,
    vectors,
    leaf_pick,
    leaf_assign,
    device_pick,
    device_assign,
    node_pick,
    node_assign,
    far_mask,
    near_lower,
    near_upper,
):
    vmem = pl.BlockSpec(memory_space=pltpu.VMEM)
    dma = pltpu.SemaphoreType.DMA
    low, high = near_lower[0], near_upper[0]
    reach = low.shape[0]
    return pl.pallas_call(
        fused,
        out_shape=jax.ShapeDtypeStruct((COLS, BLOCK), F32),
        in_specs=[pl.BlockSpec(memory_space=pltpu.HBM)] * 2 + [vmem] * 9,
        out_specs=vmem,
        scratch_shapes=[
            pltpu.VMEM((DIM, BLOCK), BF),
            pltpu.VMEM((COLS, BLOCK), BF),
            pltpu.VMEM((5, DIM, BLOCK), BF),
            pltpu.VMEM((5, COLS, BLOCK), BF),
            pltpu.VMEM((3, LPD, COLS, LEAF), BF),
            pltpu.VMEM((RING, LPD, COLS, LEAF), BF),
            pltpu.VMEM((3, 2, reach, SLOTS), jnp.int32),
            pltpu.SMEM((RING, 2, reach, SLOTS), jnp.int32),
            pltpu.VMEM((RING, LPD, LEAF, AUG), BF),
            pltpu.VMEM((3, LPD, AUG, LEAF), BF),
            pltpu.VMEM((RING, COLS, BLOCK), F32),
            pltpu.VMEM((3, COLS, BLOCK), F32),
            pltpu.VMEM((5, COLS, BLOCK), BF),
            pltpu.VMEM((5, COLS, BLOCK), BF),
            pltpu.VMEM((LEAF, LEAF), BF),
            pltpu.VMEM((LEAF, LEAF), BF),
            pltpu.VMEM((SKEL, BLOCK), BF),
            pltpu.VMEM((SKEL, SKEL), F32),
            pltpu.VMEM((NGY - 1, CHUNK, SKEL), F32),
            pltpu.VMEM((CHUNK, SKEL), F32),
            pltpu.VMEM((NGX, CHUNK, SKEL), F32),
            pltpu.VMEM((SKEL, SKEL), F32),
            pltpu.VMEM((COLS, SKEL), F32),
            pltpu.VMEM((NGY - 1, COLS, SKEL), F32),
            dma((10,)),
            dma((10,)),
            dma((6,)),
            dma((6,)),
            dma((8,)),
            dma((2,)),
            dma((4,)),
            dma((4,)),
            dma((5,)),
            dma((5,)),
            dma((NGY - 1,)),
            dma((NGY - 1,)),
            dma((NGX - 1,)),
            dma((NGX - 1,)),
            dma((NGY - 1,)),
            dma((NGY - 1,)),
            dma((NGY - 1,)),
            dma((NGY - 1,)),
        ],
        compiler_params=pltpu.CompilerParams(
            collective_id=0, has_side_effects=True, vmem_limit_bytes=56 * 2**20
        ),
        name="treecode",
    )(
        points,
        vectors,
        leaf_pick,
        leaf_assign,
        device_pick,
        device_assign,
        node_pick[0][:, None, :],
        node_assign[0][:, None, :],
        far_mask,
        low,
        high,
    )


def solution(mesh):
    placed = (
        P(None, ("gx", "gy")),
        P(None, ("gx", "gy")),
        P(("gx", "gy"), None),
        P(("gx", "gy"), None),
        P(("gx", "gy"), None),
        P(("gx", "gy"), None),
        P("gx", None, None),
        P("gx", None, None),
        P("gx", None),
        P(("gx", "gy"), None, None),
        P(("gx", "gy"), None, None),
    )
    return jax.shard_map(
        on_device, mesh=mesh, in_specs=placed, out_specs=P(None, ("gx", "gy")), check_vma=False
    )
```
